512 devices in a mesh: grp: 2 (over y), sp: 16 (over z), blk: 8 (over x), rep: 2 (over core).
Axes of the slice: x: 8, y: 2, z: 16, core: 2. Of those that a mesh axis runs over, the one named last changes fastest.
The devices are a block of a 8x8x16 slice.
Arguments:
- hidden: bfloat16 [16, 2048, 4096], P(('grp', 'blk'), 'sp'), parts along dimension 0, may hold values from -64 to 64
- queries: bfloat16 [16, 2048, 4096], P(('grp', 'blk'), 'sp', 'rep'), parts along dimension 0, may hold values from -600 to 600
- norm_gain: float32 [4096], replicated, may hold values from 0.1 to 1.9
- key_matrix: bfloat16 [4096, 1024], P('sp', 'rep'), may hold values from -0.09375 to 0.09375
- value_matrix: bfloat16 [4096, 1024], P('sp', 'rep'), may hold values from -0.09375 to 0.09375
- key_shift_bias: bfloat16 [1024], P('rep'), may hold values from -3 to 3
- value_shift_bias: bfloat16 [1024], P('rep'), may hold values from -3 to 3
- doc_lengths: int32 [16], P('grp'), parts along dimension 0, may hold values from 1 to 4097, 16384 in all
Outputs:
- attended: bfloat16 [16, 2048, 4096], P(('grp', 'blk'), 'sp', 'rep'), parts along dimension 0
The draws below stay inside these ranges and needn't reach their ends.
There are 2 independent parts, one for each index of `grp`. The reference program is written for one: setup_inputs(seed, part) draws one part's arguments, and reference() takes and returns one part's arrays. A program takes and returns all parts, laid end to end along the dimension named above; an argument that names none is the same for every part. Nothing has to cross between parts.
Inputs may be any that keep to these rules, and one draw needn't show every extreme that they name: `doc_lengths`: the lengths of the 8 documents packed in order into the sequence; they sum to 16384, and the longest is exactly 4097 tokens.
All inputs are finite; a program needn't handle non-finite values.
Results may differ from the reference program's by a relative error of at most 0.012.
The reference program's roundings to bfloat16 on the way count: a program that leaves them out, or rounds other values in their place, can miss the bound.
Values may be sent and summed in bfloat16 or wider, within the bound.
No kernel may reach another device: no remote copies, remote signals or barrier semaphores. Data moves between devices by JAX's collectives and lax.ppermute only.
A program may use at most 64 MiB of HBM per device.

```python
import math
import jax
import jax.numpy as jnp
import numpy as np
from jax import lax

MODEL_WIDTH = 4096
QUERY_HEADS = 32
KEY_VALUE_HEADS = 8
HEAD_DIMENSION = 128
DOCS = 8
CH = 2048
SEQUENCE_TOKENS = 16384
DOC_MOST = 4097


def draw_queries(key, part):
    first_key = jax.random.fold_in(jax.random.fold_in(key, 11), 0)
    full_shape = (SEQUENCE_TOKENS // CH, CH, QUERY_HEADS * HEAD_DIMENSION)
    drawn = jnp.clip(jax.random.normal(first_key, full_shape, jnp.float32), -4.0, 4.0)
    return drawn.astype(jnp.bfloat16)


def draw_hidden(key, part):
    first_key = jax.random.fold_in(jax.random.fold_in(key, 23), 0)
    full_shape = (SEQUENCE_TOKENS // CH, CH, MODEL_WIDTH)
    drawn = jnp.clip(jax.random.normal(first_key, full_shape, jnp.float32), -5.0, 5.0)
    return drawn.astype(jnp.bfloat16)


def level_of(key, dims, cuts, smallest, high):
    def one(axis_at, blocks):
        heights = jax.random.uniform(jax.random.fold_in(jax.random.fold_in(key, 6), axis_at), (blocks,), jnp.float32, smallest / len(cuts), high / len(cuts))
        return jnp.repeat(jnp.exp(heights), dims[axis_at] // blocks).reshape((-1,) + (1,) * (len(dims) - axis_at - 1))

    level = one(*cuts[0])
    for cut in cuts[1:]:
        level = level * one(*cut)
    return level


def profile(amount, total, bound, slope):
    loads = [(1 << 20) // math.isqrt(standing ** slope) + 1 for standing in range(2, amount + 1)]
    spare, given = total - bound - (amount - 1), [1] * (amount - 1)
    while spare > 0:
        candidates = [i for i in range(amount - 1) if given[i] < bound]
        pool, remaining = sum([loads[i] for i in candidates]), spare
        for i in candidates:
            extra = min(bound - given[i], max(1, remaining * loads[i] // pool), spare)
            given[i] = given[i] + extra
            spare = spare - extra
    return np.array([bound] + given)


def ragged(stream_key, amount, total, most, skew):
    if amount == 2:
        one = jax.random.randint(stream_key, (), max(1, total - most), min(most, total - 1) + 1)
        return jnp.stack([one, total - one])
    tallies = jnp.asarray(profile(amount, total, most, skew), jnp.int32)
    couples = (amount - 1) // 2
    giver, receiver = tallies[1:1 + 2 * couples:2], tallies[2:2 + 2 * couples:2]
    room = jnp.minimum(giver - 1, most - receiver)
    shifted = jax.random.randint(jax.random.fold_in(stream_key, 1), (couples,), 0, 1 << 20) % (room + 1)
    tallies = tallies.at[1:1 + 2 * couples:2].set(giver - shifted).at[2:2 + 2 * couples:2].set(receiver + shifted)
    return tallies[jax.random.permutation(jax.random.fold_in(stream_key, 2), amount)]


def centred(own_key, extent, width, most, shards=(), dtype=jnp.bfloat16):
    loudness = level_of(own_key, extent, shards, -0.22, 0.18) if shards else 1.0
    entries = jax.random.normal(own_key, extent, jnp.float32) * width * loudness
    return jnp.minimum(jnp.maximum(entries, -most), most).astype(dtype)


def setup_inputs(seed: int = 0, part: int = 0) -> dict:
    key_list = jax.random.split(jax.random.key(seed), 9)
    own_keys = jax.random.split(jax.random.fold_in(key_list[8], part), 9)
    return {
        "hidden": draw_hidden(jax.random.fold_in(jax.random.fold_in(key_list[8], part), 71), part),
        "queries": draw_queries(jax.random.fold_in(jax.random.fold_in(key_list[8], part), 71), part),
        "norm_gain": jnp.clip(1.0 + 0.18 * jax.random.normal(key_list[2], (MODEL_WIDTH,), jnp.float32), 0.1, 1.9),
        "key_matrix": centred(key_list[3], (MODEL_WIDTH, KEY_VALUE_HEADS * HEAD_DIMENSION), MODEL_WIDTH ** -0.5, 0.09375, ((0, 16), (1, 2))),
        "value_matrix": centred(key_list[4], (MODEL_WIDTH, KEY_VALUE_HEADS * HEAD_DIMENSION), MODEL_WIDTH ** -0.5, 0.09375, ((0, 16), (1, 2))),
        "key_shift_bias": centred(key_list[5], (KEY_VALUE_HEADS * HEAD_DIMENSION,), 0.5, 3.0, ((0, 2),)),
        "value_shift_bias": centred(key_list[6], (KEY_VALUE_HEADS * HEAD_DIMENSION,), 0.5, 3.0, ((0, 2),)),
        "doc_lengths": ragged(own_keys[7], DOCS, SEQUENCE_TOKENS, DOC_MOST, 2).astype(jnp.int32),
    }


EPS_VALUE = 1e-06
THETA_BASE = 1000000.0

def apply_rotation(projected, token_places):
    half_size = projected.shape[-1] // 2
    freq_index = jnp.arange(half_size).astype(jnp.float32)
    inverse = jnp.exp(freq_index * (-2.0 * math.log(THETA_BASE) / projected.shape[-1]))
    angles = token_places[:, None] * inverse[None, :]
    cosine = jnp.cos(angles)[:, None, :]
    sine = jnp.sin(angles)[:, None, :]
    first_half = projected[..., :half_size]
    second_half = projected[..., half_size:]
    return jnp.concatenate([first_half * cosine - second_half * sine, second_half * cosine + first_half * sine], axis=-1)

def doc_index(token_places, doc_lengths):
    ending = jnp.cumsum(doc_lengths).astype(jnp.int32)
    return lax.optimization_barrier(jnp.sum((token_places[:, None] >= ending[None, :]).astype(jnp.int32), axis=1))

def reference(hidden, queries, norm_gain, key_matrix, value_matrix, key_shift_bias, value_shift_bias, doc_lengths):
    rows_all = hidden.reshape(SEQUENCE_TOKENS, MODEL_WIDTH).astype(jnp.float32)
    row_scale = lax.rsqrt(lax.optimization_barrier(jnp.mean(rows_all * rows_all, axis=1, keepdims=True)) + EPS_VALUE)
    normed = (rows_all * row_scale * norm_gain.astype(jnp.float32)).astype(jnp.bfloat16)
    token_places = jnp.arange(SEQUENCE_TOKENS).astype(jnp.int32)
    key_projector = jnp.dot(normed, key_matrix, preferred_element_type=jnp.float32) + key_shift_bias.astype(jnp.float32)
    value_projector = jnp.dot(normed, value_matrix, preferred_element_type=jnp.float32) + value_shift_bias.astype(jnp.float32)
    key_vectors = apply_rotation(key_projector.reshape(SEQUENCE_TOKENS, KEY_VALUE_HEADS, HEAD_DIMENSION), token_places.astype(jnp.float32)).astype(jnp.bfloat16)
    value_vectors = value_projector.reshape(SEQUENCE_TOKENS, KEY_VALUE_HEADS, HEAD_DIMENSION).astype(jnp.bfloat16)
    segment = doc_index(token_places, doc_lengths)
    visible = (token_places[None, :] <= token_places[:, None]) & (segment[None, :] == segment[:, None])
    query_heads = queries.reshape(SEQUENCE_TOKENS, QUERY_HEADS, HEAD_DIMENSION).transpose(1, 0, 2)
    heads_of_keys = jnp.repeat(key_vectors.transpose(1, 0, 2), QUERY_HEADS // KEY_VALUE_HEADS, axis=0)
    heads_of_values = jnp.repeat(value_vectors.transpose(1, 0, 2), QUERY_HEADS // KEY_VALUE_HEADS, axis=0)
    scale_factor = 1.0 / math.sqrt(HEAD_DIMENSION)

    def one_head(triple):
        query_rows, key_rows, value_rows = triple
        scores = jnp.dot(query_rows, key_rows.T, preferred_element_type=jnp.float32) * scale_factor
        scores = jnp.where(visible, scores, -1e+30)
        largest = lax.optimization_barrier(jnp.max(scores, axis=1, keepdims=True))
        weights = jnp.where(visible, jnp.exp(scores - largest), 0.0).astype(jnp.bfloat16)
        total = lax.optimization_barrier(jnp.sum(weights.astype(jnp.float32), axis=1, keepdims=True))
        summed = jnp.dot(weights, value_rows, preferred_element_type=jnp.float32)
        return (summed / total).astype(jnp.bfloat16)
    result = lax.map(one_head, (query_heads, heads_of_keys, heads_of_values))
    return result.transpose(1, 0, 2).reshape(SEQUENCE_TOKENS // CH, CH, QUERY_HEADS * HEAD_DIMENSION)
```

```python
import functools
import math

import jax
import jax.numpy as jnp
from jax import lax
from jax.experimental import pallas as pl
from jax.experimental.pallas import tpu as pltpu
from jax.sharding import PartitionSpec as P

HEAD = 128
EPS_VALUE = 1e-06
THETA_BASE = 1000000.0
START_MAX = -1e30
HIDDEN_SCORE = -3e38
EXP2_SCALE = math.log2(math.e) / math.sqrt(HEAD)
PIECE = 512
TILE = 128
ROWS = 256


def apply_rotation(projected, token_places):
    half_size = projected.shape[-1] // 2
    freq_index = jnp.arange(half_size).astype(jnp.float32)
    inverse = jnp.exp(freq_index * (-2.0 * math.log(THETA_BASE) / projected.shape[-1]))
    angles = token_places[:, None] * inverse[None, :]
    cosine = jnp.cos(angles)[:, None, :]
    sine = jnp.sin(angles)[:, None, :]
    first_half = projected[..., :half_size]
    second_half = projected[..., half_size:]
    return jnp.concatenate(
        [first_half * cosine - second_half * sine, second_half * cosine + first_half * sine],
        axis=-1,
    )


def attention_kernel(blocks, heads, first, last, info, docs, q_ref, *refs):
    keys, values = refs[:blocks], refs[blocks : 2 * blocks]
    rest = list(refs[2 * blocks :])
    if not first:
        max_in, sum_in = rest[0], rest[1]
        rest = rest[2:]
    if last:
        out_ref = rest[0]
        max_ref, sum_ref = rest[1], rest[2]
        rest = rest[3:]
    else:
        max_ref, sum_ref = rest[0], rest[1]
        rest = rest[2:]
    stacked = rest[0]
    bounds = rest[1]
    tiles = q_ref.shape[0] // TILE
    count = docs.shape[0]
    pieces = keys[0].shape[0] // PIECE
    query_base = info[0]

    ends = []
    total = 0
    for d in range(count):
        total = total + docs[d]
        ends.append(total)

    def start_of(place):
        begin = 0
        for end in ends:
            begin = jnp.where(end <= place, end, begin)
        return begin

    for i in range(tiles):
        low = query_base + i * TILE
        bounds[2 * i] = start_of(low)
        bounds[2 * i + 1] = start_of(low + TILE - 1)
        for h in range(heads):
            stacked[i, h * TILE : (h + 1) * TILE, :] = q_ref[
                i * TILE : (i + 1) * TILE, h * HEAD : (h + 1) * HEAD
            ]
    if first:
        max_ref[...] = jnp.full(max_ref.shape, START_MAX, jnp.float32)
        sum_ref[...] = jnp.zeros(sum_ref.shape, jnp.float32)
    else:
        max_ref[...] = max_in[...]
        sum_ref[...] = sum_in[...]

    def step(key_ref, value_ref, piece, i, low, key_low, masked):
        key_rows = pl.ds(pl.multiple_of(piece * PIECE, PIECE), PIECE)
        key = key_ref[key_rows, :]
        value = jnp.concatenate(
            [value_ref[key_rows, :], jnp.ones((PIECE, HEAD), jnp.bfloat16)], axis=1
        )
        visible = None
        if masked:
            row_place = low + lax.broadcasted_iota(jnp.int32, (TILE, HEAD), 0)
            begin = jnp.zeros((TILE, HEAD), jnp.int32)
            for end in ends:
                begin = jnp.where(row_place >= end, end, begin)
            lanes = lax.broadcasted_iota(jnp.int32, (TILE, HEAD), 1)
            parts = []
            for part in range(PIECE // HEAD):
                key_place = lanes + (key_low + part * HEAD)
                parts.append((key_place <= row_place) & (key_place >= begin))
            visible = jnp.concatenate(parts, axis=1)
        for r in range(heads * TILE // ROWS):
            rows = slice(r * ROWS, (r + 1) * ROWS)
            scores = lax.dot_general(
                stacked[i, rows, :],
                key,
                (((1,), (1,)), ((), ())),
                preferred_element_type=jnp.float32,
            )
            if masked:
                scores = jnp.concatenate(
                    [
                        jnp.where(visible, scores[k * TILE : (k + 1) * TILE], HIDDEN_SCORE)
                        for k in range(ROWS // TILE)
                    ],
                    axis=0,
                )
            old_max = max_ref[i, rows, :]
            new_max = jnp.maximum(old_max, jnp.max(scores, axis=1, keepdims=True))
            factor = jnp.exp2((old_max - new_max) * EXP2_SCALE)
            weights = jnp.exp2(
                (scores - jnp.concatenate([new_max] * (PIECE // HEAD), axis=1)) * EXP2_SCALE
            ).astype(jnp.bfloat16)
            added = lax.dot_general(
                weights, value, (((1,), (0,)), ((), ())), preferred_element_type=jnp.float32
            )
            sum_ref[i, rows, :] = (
                sum_ref[i, rows, :] * jnp.concatenate([factor, factor], axis=1) + added
            )
            max_ref[i, rows, :] = new_max

    for j in range(blocks):
        key_base = info[1 + j]

        def over_pieces(piece, carry, j=j, key_base=key_base):
            key_low = key_base + piece * PIECE

            def over_tiles(i, inner):
                low = query_base + i * TILE
                reached = (key_low <= low + TILE - 1) & (
                    key_low + PIECE - 1 >= bounds[2 * i]
                )
                whole = (key_low + PIECE - 1 <= low) & (key_low >= bounds[2 * i + 1])

                @pl.when(reached & whole)
                def _():
                    step(keys[j], values[j], piece, i, low, key_low, False)

                @pl.when(reached & jnp.logical_not(whole))
                def _():
                    step(keys[j], values[j], piece, i, low, key_low, True)

                return inner

            return lax.fori_loop(0, tiles, over_tiles, carry)

        lax.fori_loop(0, pieces, over_pieces, 0)

    if last:
        for i in range(tiles):
            for h in range(heads):
                rows = slice(h * TILE, (h + 1) * TILE)
                out_ref[i * TILE : (i + 1) * TILE, h * HEAD : (h + 1) * HEAD] = (
                    sum_ref[i, rows, :HEAD] / sum_ref[i, rows, HEAD:]
                ).astype(jnp.bfloat16)


def attend(info, docs, query, keys, values, state, last):
    tokens = query.shape[0]
    heads = query.shape[1] // HEAD
    tiles = tokens // TILE
    blocks = len(keys)
    first = state is None
    max_shape = (tiles, heads * TILE, HEAD)
    sum_shape = (tiles, heads * TILE, 2 * HEAD)
    vmem = pl.BlockSpec(memory_space=pltpu.VMEM)
    smem = pl.BlockSpec(memory_space=pltpu.SMEM)
    held = [pltpu.VMEM(max_shape, jnp.float32), pltpu.VMEM(sum_shape, jnp.float32)]
    scratch = [
        pltpu.VMEM((tiles, heads * TILE, HEAD), jnp.bfloat16),
        pltpu.SMEM((2 * tiles,), jnp.int32),
    ]
    if last:
        out_shape = jax.ShapeDtypeStruct((tokens, heads * HEAD), jnp.bfloat16)
        out_specs = vmem
        scratch = held + scratch
    else:
        out_shape = (
            jax.ShapeDtypeStruct(max_shape, jnp.float32),
            jax.ShapeDtypeStruct(sum_shape, jnp.float32),
        )
        out_specs = (vmem, vmem)
    operands = [query, *keys, *values] + ([] if first else list(state))
    pairs = tokens * heads * keys[0].shape[0] * blocks
    return pl.pallas_call(
        functools.partial(attention_kernel, blocks, heads, first, last),
        out_shape=out_shape,
        in_specs=[smem, smem] + [vmem] * len(operands),
        out_specs=out_specs,
        scratch_shapes=scratch,
        name="attend_last" if last else "attend_first",
        cost_estimate=pl.CostEstimate(
            flops=pairs * 4 * HEAD, bytes_accessed=4 << 20, transcendentals=pairs
        ),
        compiler_params=pltpu.CompilerParams(vmem_limit_bytes=40 << 20),
    )(info, docs, *operands)


def on_device(
    hidden,
    queries,
    norm_gain,
    key_matrix,
    value_matrix,
    key_shift_bias,
    value_shift_bias,
    doc_lengths,
):
    sp_count = lax.axis_size("sp")
    blk_count = lax.axis_size("blk")
    sp_place = lax.axis_index("sp")
    blk_place = lax.axis_index("blk")
    rep_place = lax.axis_index("rep")
    local_rows = hidden.shape[1]
    width = hidden.shape[2]
    span_rows = local_rows * sp_count
    kv_local = key_matrix.shape[1] // HEAD
    quads = sp_count // kv_local
    quad_rows = local_rows * kv_local
    side = blk_place % 2
    half_heads = kv_local // 2
    half_columns = half_heads * HEAD

    near = [[q * kv_local + i for i in range(kv_local)] for q in range(quads)]
    swap = [(b, b ^ 1) for b in range(blk_count)]
    ahead = [(b, (b + 1) % blk_count) for b in range(blk_count)]
    behind = [((b + 1) % blk_count, b) for b in range(blk_count)]

    picked = jnp.concatenate(
        [
            lax.dynamic_slice_in_dim(key_matrix, side * half_columns, half_columns, 1),
            lax.dynamic_slice_in_dim(value_matrix, side * half_columns, half_columns, 1),
        ],
        axis=1,
    )
    weight = lax.all_gather(picked, "sp", axis=0, tiled=True)

    rows_all = hidden[0].astype(jnp.float32)
    row_scale = lax.rsqrt(jnp.mean(rows_all * rows_all, axis=1, keepdims=True) + EPS_VALUE)
    normed = (rows_all * row_scale * norm_gain).astype(jnp.bfloat16)
    half_width = width // 2
    mine = lax.dynamic_slice_in_dim(normed, rep_place * half_width, half_width, 1)
    theirs = lax.ppermute(mine, "blk", swap)
    theirs_other = lax.ppermute(theirs, "rep", [(0, 1), (1, 0)])
    is_low = rep_place == 0
    partner = jnp.concatenate(
        [
            jnp.where(is_low, theirs, theirs_other),
            jnp.where(is_low, theirs_other, theirs),
        ],
        axis=1,
    )
    both = jnp.concatenate([normed, partner], axis=0)

    query_moved = lax.ppermute(queries[0], "blk", behind)
    query = lax.all_to_all(
        query_moved, "sp", split_axis=1, concat_axis=0, tiled=True, axis_index_groups=near
    )

    projected = jnp.dot(both, weight, preferred_element_type=jnp.float32)
    bias = jnp.concatenate(
        [
            lax.dynamic_slice_in_dim(key_shift_bias, side * half_columns, half_columns, 0),
            lax.dynamic_slice_in_dim(value_shift_bias, side * half_columns, half_columns, 0),
        ]
    ).astype(jnp.float32)
    projected = projected + bias
    local_places = sp_place * local_rows + jnp.arange(local_rows)
    places = jnp.concatenate(
        [local_places + blk_place * span_rows, local_places + (blk_place ^ 1) * span_rows]
    )
    keys_new = apply_rotation(
        projected[:, :half_columns].reshape(2 * local_rows, half_heads, HEAD),
        places.astype(jnp.float32),
    ).astype(jnp.bfloat16)
    values_new = (
        projected[:, half_columns:]
        .reshape(2 * local_rows, half_heads, HEAD)
        .astype(jnp.bfloat16)
    )
    pair_new = jnp.concatenate([keys_new, values_new], axis=2).reshape(
        2 * local_rows, half_heads * 2 * HEAD
    )
    kept = pair_new[:local_rows]
    other = lax.ppermute(pair_new[local_rows:], "blk", swap)
    even = side == 0
    all_heads = jnp.concatenate(
        [jnp.where(even, kept, other), jnp.where(even, other, kept)], axis=1
    )
    def to_heads(part):
        one = all_heads.reshape(local_rows, kv_local, 2 * HEAD)[:, :, part * HEAD : (part + 1) * HEAD]
        sent = jnp.tile(one.reshape(local_rows, kv_local * HEAD), (1, quads))
        return lax.all_to_all(sent, "sp", split_axis=1, concat_axis=0, tiled=True)

    key_block = to_heads(0)
    value_block = to_heads(1)
    key_next = lax.ppermute(key_block, "blk", behind)
    key_prior = lax.ppermute(key_block, "blk", ahead)
    value_next = lax.ppermute(value_block, "blk", behind)
    value_prior = lax.ppermute(value_block, "blk", ahead)

    query_block = (blk_place + 1) % blk_count
    base = query_block * span_rows
    query_base = base + sp_place // kv_local * quad_rows
    info_first = jnp.stack([query_base, base - span_rows]).astype(jnp.int32)
    info_last = jnp.stack([query_base, base, base - 2 * span_rows]).astype(jnp.int32)
    state = attend(info_first, doc_lengths, query, [key_block], [value_block], None, False)
    result = attend(
        info_last,
        doc_lengths,
        query,
        [key_next, key_prior],
        [value_next, value_prior],
        state,
        True,
    )
    spread = lax.all_to_all(
        result, "sp", split_axis=0, concat_axis=1, tiled=True, axis_index_groups=near
    )
    return lax.ppermute(spread, "blk", ahead)[None]


def solution(mesh):
    in_specs = (
        P(("grp", "blk"), "sp", None),
        P(("grp", "blk"), "sp", "rep"),
        P(),
        P("sp", "rep"),
        P("sp", "rep"),
        P("rep"),
        P("rep"),
        P("grp"),
    )
    out_specs = P(("grp", "blk"), "sp", "rep")
    return jax.shard_map(
        on_device, mesh=mesh, in_specs=in_specs, out_specs=out_specs, check_vma=False
    )
```

```python
import functools
import math

import jax
import jax.numpy as jnp
from jax import lax
from jax.experimental import pallas as pl
from jax.experimental.pallas import tpu as pltpu
from jax.sharding import PartitionSpec as P

HEAD = 128
EPS_VALUE = 1e-06
THETA_BASE = 1000000.0
START_MAX = -1e30
HIDDEN_SCORE = -3e38
EXP2_SCALE = math.log2(math.e) / math.sqrt(HEAD)
PIECE = 512
TILE = 128
ROWS = 256


def apply_rotation(projected, token_places):
    half_size = projected.shape[-1] // 2
    freq_index = jnp.arange(half_size).astype(jnp.float32)
    inverse = jnp.exp(freq_index * (-2.0 * math.log(THETA_BASE) / projected.shape[-1]))
    angles = token_places[:, None] * inverse[None, :]
    cosine = jnp.cos(angles)[:, None, :]
    sine = jnp.sin(angles)[:, None, :]
    first_half = projected[..., :half_size]
    second_half = projected[..., half_size:]
    return jnp.concatenate(
        [first_half * cosine - second_half * sine, second_half * cosine + first_half * sine],
        axis=-1,
    )


def attention_kernel(blocks, heads, first, last, info, docs, q_ref, *refs):
    keys, values = refs[:blocks], refs[blocks : 2 * blocks]
    rest = list(refs[2 * blocks :])
    if not first:
        max_in, sum_in = rest[0], rest[1]
        rest = rest[2:]
    if last:
        out_ref = rest[0]
        max_ref, sum_ref = rest[1], rest[2]
        rest = rest[3:]
    else:
        max_ref, sum_ref = rest[0], rest[1]
        rest = rest[2:]
    stacked = rest[0]
    bounds = rest[1]
    tiles = q_ref.shape[0] // TILE
    count = docs.shape[0]
    pieces = keys[0].shape[0] // PIECE
    query_base = info[0]

    ends = []
    total = 0
    for d in range(count):
        total = total + docs[d]
        ends.append(total)

    def start_of(place):
        begin = 0
        for end in ends:
            begin = jnp.where(end <= place, end, begin)
        return begin

    for i in range(tiles):
        low = query_base + i * TILE
        bounds[2 * i] = start_of(low)
        bounds[2 * i + 1] = start_of(low + TILE - 1)
        for h in range(heads):
            stacked[i, h * TILE : (h + 1) * TILE, :] = q_ref[
                i * TILE : (i + 1) * TILE, h * HEAD : (h + 1) * HEAD
            ]
    if first:
        max_ref[...] = jnp.full(max_ref.shape, START_MAX, jnp.float32)
        sum_ref[...] = jnp.zeros(sum_ref.shape, jnp.float32)
    else:
        max_ref[...] = max_in[...]
        sum_ref[...] = sum_in[...]

    def step(key_ref, value_ref, piece, i, low, key_low, masked):
        key_rows = pl.ds(pl.multiple_of(piece * PIECE, PIECE), PIECE)
        key = key_ref[key_rows, :]
        value = jnp.concatenate(
            [value_ref[key_rows, :], jnp.ones((PIECE, HEAD), jnp.bfloat16)], axis=1
        )
        visible = None
        if masked:
            row_place = low + lax.broadcasted_iota(jnp.int32, (TILE, HEAD), 0)
            begin = jnp.zeros((TILE, HEAD), jnp.int32)
            for end in ends:
                begin = jnp.where(row_place >= end, end, begin)
            lanes = lax.broadcasted_iota(jnp.int32, (TILE, HEAD), 1)
            parts = []
            for part in range(PIECE // HEAD):
                key_place = lanes + (key_low + part * HEAD)
                parts.append((key_place <= row_place) & (key_place >= begin))
            visible = jnp.concatenate(parts, axis=1)
        for r in range(heads * TILE // ROWS):
            rows = slice(r * ROWS, (r + 1) * ROWS)
            scores = lax.dot_general(
                stacked[i, rows, :],
                key,
                (((1,), (1,)), ((), ())),
                preferred_element_type=jnp.float32,
            )
            if masked:
                scores = jnp.concatenate(
                    [
                        jnp.where(visible, scores[k * TILE : (k + 1) * TILE], HIDDEN_SCORE)
                        for k in range(ROWS // TILE)
                    ],
                    axis=0,
                )
            old_max = max_ref[i, rows, :]
            new_max = jnp.maximum(old_max, jnp.max(scores, axis=1, keepdims=True))
            factor = jnp.exp2((old_max - new_max) * EXP2_SCALE)
            weights = jnp.exp2(
                (scores - jnp.concatenate([new_max] * (PIECE // HEAD), axis=1)) * EXP2_SCALE
            ).astype(jnp.bfloat16)
            added = lax.dot_general(
                weights, value, (((1,), (0,)), ((), ())), preferred_element_type=jnp.float32
            )
            sum_ref[i, rows, :] = (
                sum_ref[i, rows, :] * jnp.concatenate([factor, factor], axis=1) + added
            )
            max_ref[i, rows, :] = new_max

    for j in range(blocks):
        key_base = info[1 + j]

        def over_pieces(piece, carry, j=j, key_base=key_base):
            key_low = key_base + piece * PIECE

            def over_tiles(i, inner):
                low = query_base + i * TILE
                reached = (key_low <= low + TILE - 1) & (
                    key_low + PIECE - 1 >= bounds[2 * i]
                )
                whole = (key_low + PIECE - 1 <= low) & (key_low >= bounds[2 * i + 1])

                @pl.when(reached & whole)
                def _():
                    step(keys[j], values[j], piece, i, low, key_low, False)

                @pl.when(reached & jnp.logical_not(whole))
                def _():
                    step(keys[j], values[j], piece, i, low, key_low, True)

                return inner

            return lax.fori_loop(0, tiles, over_tiles, carry)

        lax.fori_loop(0, pieces, over_pieces, 0)

    if last:
        for i in range(tiles):
            for h in range(heads):
                rows = slice(h * TILE, (h + 1) * TILE)
                out_ref[i * TILE : (i + 1) * TILE, h * HEAD : (h + 1) * HEAD] = (
                    sum_ref[i, rows, :HEAD] / sum_ref[i, rows, HEAD:]
                ).astype(jnp.bfloat16)


def attend(info, docs, query, keys, values, state, last):
    tokens = query.shape[0]
    heads = query.shape[1] // HEAD
    tiles = tokens // TILE
    blocks = len(keys)
    first = state is None
    max_shape = (tiles, heads * TILE, HEAD)
    sum_shape = (tiles, heads * TILE, 2 * HEAD)
    vmem = pl.BlockSpec(memory_space=pltpu.VMEM)
    smem = pl.BlockSpec(memory_space=pltpu.SMEM)
    held = [pltpu.VMEM(max_shape, jnp.float32), pltpu.VMEM(sum_shape, jnp.float32)]
    scratch = [
        pltpu.VMEM((tiles, heads * TILE, HEAD), jnp.bfloat16),
        pltpu.SMEM((2 * tiles,), jnp.int32),
    ]
    if last:
        out_shape = jax.ShapeDtypeStruct((tokens, heads * HEAD), jnp.bfloat16)
        out_specs = vmem
        scratch = held + scratch
    else:
        out_shape = (
            jax.ShapeDtypeStruct(max_shape, jnp.float32),
            jax.ShapeDtypeStruct(sum_shape, jnp.float32),
        )
        out_specs = (vmem, vmem)
    operands = [query, *keys, *values] + ([] if first else list(state))
    pairs = tokens * heads * keys[0].shape[0] * blocks
    return pl.pallas_call(
        functools.partial(attention_kernel, blocks, heads, first, last),
        out_shape=out_shape,
        in_specs=[smem, smem] + [vmem] * len(operands),
        out_specs=out_specs,
        scratch_shapes=scratch,
        name="attend_last" if last else "attend_first",
        cost_estimate=pl.CostEstimate(
            flops=pairs * 4 * HEAD, bytes_accessed=4 << 20, transcendentals=pairs
        ),
        compiler_params=pltpu.CompilerParams(vmem_limit_bytes=40 << 20),
    )(info, docs, *operands)


def on_device(
    hidden,
    queries,
    norm_gain,
    key_matrix,
    value_matrix,
    key_shift_bias,
    value_shift_bias,
    doc_lengths,
):
    sp_count = lax.axis_size("sp")
    blk_count = lax.axis_size("blk")
    sp_place = lax.axis_index("sp")
    blk_place = lax.axis_index("blk")
    rep_place = lax.axis_index("rep")
    local_rows = hidden.shape[1]
    width = hidden.shape[2]
    span_rows = local_rows * sp_count
    kv_local = key_matrix.shape[1] // HEAD
    quads = sp_count // kv_local
    quad_rows = local_rows * kv_local
    side = blk_place % 2
    half_heads = kv_local // 2
    half_columns = half_heads * HEAD

    near = [[q * kv_local + i for i in range(kv_local)] for q in range(quads)]
    swap = [(b, b ^ 1) for b in range(blk_count)]
    ahead = [(b, (b + 1) % blk_count) for b in range(blk_count)]
    behind = [((b + 1) % blk_count, b) for b in range(blk_count)]

    picked = jnp.concatenate(
        [
            lax.dynamic_slice_in_dim(key_matrix, side * half_columns, half_columns, 1),
            lax.dynamic_slice_in_dim(value_matrix, side * half_columns, half_columns, 1),
        ],
        axis=1,
    )
    weight = lax.all_gather(picked, "sp", axis=0, tiled=True)

    rows_all = hidden[0].astype(jnp.float32)
    row_scale = lax.rsqrt(jnp.mean(rows_all * rows_all, axis=1, keepdims=True) + EPS_VALUE)
    normed = (rows_all * row_scale * norm_gain).astype(jnp.bfloat16)
    half_width = width // 2
    mine = lax.dynamic_slice_in_dim(normed, rep_place * half_width, half_width, 1)
    theirs = lax.ppermute(mine, "blk", swap)
    theirs_other = lax.ppermute(theirs, "rep", [(0, 1), (1, 0)])
    is_low = rep_place == 0
    partner = jnp.concatenate(
        [
            jnp.where(is_low, theirs, theirs_other),
            jnp.where(is_low, theirs_other, theirs),
        ],
        axis=1,
    )
    both = jnp.concatenate([normed, partner], axis=0)

    query_moved = lax.ppermute(queries[0], "blk", behind)
    query = lax.all_to_all(
        query_moved, "sp", split_axis=1, concat_axis=0, tiled=True, axis_index_groups=near
    )

    both, query = lax.optimization_barrier((both, query))
    projected = jnp.dot(both, weight, preferred_element_type=jnp.float32)
    bias = jnp.concatenate(
        [
            lax.dynamic_slice_in_dim(key_shift_bias, side * half_columns, half_columns, 0),
            lax.dynamic_slice_in_dim(value_shift_bias, side * half_columns, half_columns, 0),
        ]
    ).astype(jnp.float32)
    projected = projected + bias
    local_places = sp_place * local_rows + jnp.arange(local_rows)
    places = jnp.concatenate(
        [local_places + blk_place * span_rows, local_places + (blk_place ^ 1) * span_rows]
    )
    keys_new = apply_rotation(
        projected[:, :half_columns].reshape(2 * local_rows, half_heads, HEAD),
        places.astype(jnp.float32),
    ).astype(jnp.bfloat16)
    values_new = (
        projected[:, half_columns:]
        .reshape(2 * local_rows, half_heads, HEAD)
        .astype(jnp.bfloat16)
    )
    pair_new = jnp.concatenate([keys_new, values_new], axis=2).reshape(
        2 * local_rows, half_heads * 2 * HEAD
    )
    kept = pair_new[:local_rows]
    other = lax.ppermute(pair_new[local_rows:], "blk", swap)
    even = side == 0
    all_heads = jnp.concatenate(
        [jnp.where(even, kept, other), jnp.where(even, other, kept)], axis=1
    )
    def to_heads(part):
        one = all_heads.reshape(local_rows, kv_local, 2 * HEAD)[:, :, part * HEAD : (part + 1) * HEAD]
        sent = jnp.tile(one.reshape(local_rows, kv_local * HEAD), (1, quads))
        return lax.all_to_all(sent, "sp", split_axis=1, concat_axis=0, tiled=True)

    key_block = to_heads(0)
    value_block = to_heads(1)
    key_next = lax.ppermute(key_block, "blk", behind)
    key_prior = lax.ppermute(key_block, "blk", ahead)
    value_next = lax.ppermute(value_block, "blk", behind)
    value_prior = lax.ppermute(value_block, "blk", ahead)

    query_block = (blk_place + 1) % blk_count
    base = query_block * span_rows
    query_base = base + sp_place // kv_local * quad_rows
    info_first = jnp.stack([query_base, base - span_rows]).astype(jnp.int32)
    info_last = jnp.stack([query_base, base, base - 2 * span_rows]).astype(jnp.int32)
    state = attend(info_first, doc_lengths, query, [key_block], [value_block], None, False)
    result = attend(
        info_last,
        doc_lengths,
        query,
        [key_next, key_prior],
        [value_next, value_prior],
        state,
        True,
    )
    spread = lax.all_to_all(
        result, "sp", split_axis=0, concat_axis=1, tiled=True, axis_index_groups=near
    )
    return lax.ppermute(spread, "blk", ahead)[None]


def solution(mesh):
    in_specs = (
        P(("grp", "blk"), "sp", None),
        P(("grp", "blk"), "sp", "rep"),
        P(),
        P("sp", "rep"),
        P("sp", "rep"),
        P("rep"),
        P("rep"),
        P("grp"),
    )
    out_specs = P(("grp", "blk"), "sp", "rep")
    return jax.shard_map(
        on_device, mesh=mesh, in_specs=in_specs, out_specs=out_specs, check_vma=False
    )
```

```python
import functools
import math

import jax
import jax.numpy as jnp
from jax import lax
from jax.experimental import pallas as pl
from jax.experimental.pallas import tpu as pltpu
from jax.sharding import PartitionSpec as P

HEAD = 128
EPS_VALUE = 1e-06
THETA_BASE = 1000000.0
START_MAX = -1e30
HIDDEN_SCORE = -3e38
EXP2_SCALE = math.log2(math.e) / math.sqrt(HEAD)
PIECE = 1024
TILE = 128
LEAD = 2
ROWS = 256


def apply_rotation(projected, token_places):
    half_size = projected.shape[-1] // 2
    freq_index = jnp.arange(half_size).astype(jnp.float32)
    inverse = jnp.exp(freq_index * (-2.0 * math.log(THETA_BASE) / projected.shape[-1]))
    angles = token_places[:, None] * inverse[None, :]
    cosine = jnp.cos(angles)[:, None, :]
    sine = jnp.sin(angles)[:, None, :]
    first_half = projected[..., :half_size]
    second_half = projected[..., half_size:]
    return jnp.concatenate(
        [first_half * cosine - second_half * sine, second_half * cosine + first_half * sine],
        axis=-1,
    )


def attention_kernel(blocks, heads, first, last, info, docs, q_ref, *refs):
    keys, values = refs[:blocks], refs[blocks : 2 * blocks]
    rest = list(refs[2 * blocks :])
    if not first:
        max_in, sum_in = rest[0], rest[1]
        rest = rest[2:]
    if last:
        out_ref = rest[0]
        max_ref, sum_ref = rest[1], rest[2]
        rest = rest[3:]
    else:
        max_ref, sum_ref = rest[0], rest[1]
        rest = rest[2:]
    stacked = rest[0]
    bounds = rest[1]
    tiles = q_ref.shape[0] // TILE
    count = docs.shape[0]
    pieces = keys[0].shape[0] // PIECE
    query_base = info[0]

    ends = []
    total = 0
    for d in range(count):
        total = total + docs[d]
        ends.append(total)

    def start_of(place):
        begin = 0
        for end in ends:
            begin = jnp.where(end <= place, end, begin)
        return begin

    for i in range(tiles):
        low = query_base + i * TILE
        bounds[2 * i] = start_of(low)
        bounds[2 * i + 1] = start_of(low + TILE - 1)
        for h in range(heads):
            stacked[i, h * TILE : (h + 1) * TILE, :] = q_ref[
                i * TILE : (i + 1) * TILE, h * HEAD : (h + 1) * HEAD
            ]
    if first:
        max_ref[...] = jnp.full(max_ref.shape, START_MAX, jnp.float32)
        sum_ref[...] = jnp.zeros(sum_ref.shape, jnp.float32)
    else:
        max_ref[...] = max_in[...]
        sum_ref[...] = sum_in[...]

    def step(key_ref, value_ref, piece, i, low, key_low, masked):
        key_rows = pl.ds(pl.multiple_of(piece * PIECE, PIECE), PIECE)
        key = key_ref[key_rows, :]
        value = jnp.concatenate(
            [value_ref[key_rows, :], jnp.ones((PIECE, HEAD), jnp.bfloat16)], axis=1
        )
        visible = None
        if masked:
            row_place = low + lax.broadcasted_iota(jnp.int32, (TILE, HEAD), 0)
            begin = jnp.zeros((TILE, HEAD), jnp.int32)
            for end in ends:
                begin = jnp.where(row_place >= end, end, begin)
            lanes = lax.broadcasted_iota(jnp.int32, (TILE, HEAD), 1)
            parts = []
            for part in range(PIECE // HEAD):
                key_place = lanes + (key_low + part * HEAD)
                parts.append((key_place <= row_place) & (key_place >= begin))
            visible = jnp.concatenate(parts, axis=1)
        chunks = heads * TILE // ROWS

        def scores_of(r):
            scores = lax.dot_general(
                stacked[i, r * ROWS : (r + 1) * ROWS, :],
                key,
                (((1,), (1,)), ((), ())),
                preferred_element_type=jnp.float32,
            )
            if masked:
                scores = jnp.concatenate(
                    [
                        jnp.where(visible, scores[k * TILE : (k + 1) * TILE], HIDDEN_SCORE)
                        for k in range(ROWS // TILE)
                    ],
                    axis=0,
                )
            return scores

        ready = [scores_of(r) for r in range(min(LEAD, chunks))]
        for r in range(chunks):
            rows = slice(r * ROWS, (r + 1) * ROWS)
            scores = ready.pop(0)
            if r + LEAD < chunks:
                ready.append(scores_of(r + LEAD))
            old_max = max_ref[i, rows, :]
            new_max = jnp.maximum(old_max, jnp.max(scores, axis=1, keepdims=True))
            factor = jnp.exp2((old_max - new_max) * EXP2_SCALE)
            weights = jnp.exp2(
                (scores - jnp.concatenate([new_max] * (PIECE // HEAD), axis=1)) * EXP2_SCALE
            ).astype(jnp.bfloat16)
            added = lax.dot_general(
                weights, value, (((1,), (0,)), ((), ())), preferred_element_type=jnp.float32
            )
            sum_ref[i, rows, :] = (
                sum_ref[i, rows, :] * jnp.concatenate([factor, factor], axis=1) + added
            )
            max_ref[i, rows, :] = new_max

    for j in range(blocks):
        key_base = info[1 + j]

        def over_pieces(piece, carry, j=j, key_base=key_base):
            key_low = key_base + piece * PIECE

            def over_tiles(i, inner):
                low = query_base + i * TILE
                reached = (key_low <= low + TILE - 1) & (
                    key_low + PIECE - 1 >= bounds[2 * i]
                )
                whole = (key_low + PIECE - 1 <= low) & (key_low >= bounds[2 * i + 1])

                @pl.when(reached & whole)
                def _():
                    step(keys[j], values[j], piece, i, low, key_low, False)

                @pl.when(reached & jnp.logical_not(whole))
                def _():
                    step(keys[j], values[j], piece, i, low, key_low, True)

                return inner

            return lax.fori_loop(0, tiles, over_tiles, carry)

        lax.fori_loop(0, pieces, over_pieces, 0)

    if last:
        for i in range(tiles):
            for h in range(heads):
                rows = slice(h * TILE, (h + 1) * TILE)
                out_ref[i * TILE : (i + 1) * TILE, h * HEAD : (h + 1) * HEAD] = (
                    sum_ref[i, rows, :HEAD] / sum_ref[i, rows, HEAD:]
                ).astype(jnp.bfloat16)


def attend(info, docs, query, keys, values, state, last, part=0, parts=1):
    tokens = query.shape[0] // parts
    heads = query.shape[1] // HEAD
    tiles = tokens // TILE
    blocks = len(keys)
    first = state is None
    max_shape = (tiles, heads * TILE, HEAD)
    sum_shape = (tiles, heads * TILE, 2 * HEAD)
    vmem = pl.BlockSpec(memory_space=pltpu.VMEM)
    smem = pl.BlockSpec(memory_space=pltpu.SMEM)
    held = [pltpu.VMEM(max_shape, jnp.float32), pltpu.VMEM(sum_shape, jnp.float32)]
    scratch = [
        pltpu.VMEM((tiles, heads * TILE, HEAD), jnp.bfloat16),
        pltpu.SMEM((2 * tiles,), jnp.int32),
    ]
    if last:
        out_shape = jax.ShapeDtypeStruct((tokens, heads * HEAD), jnp.bfloat16)
        out_specs = vmem
        scratch = held + scratch
    else:
        out_shape = (
            jax.ShapeDtypeStruct(max_shape, jnp.float32),
            jax.ShapeDtypeStruct(sum_shape, jnp.float32),
        )
        out_specs = (vmem, vmem)
    operands = [query, *keys, *values] + ([] if first else list(state))
    specs = [pl.BlockSpec((tokens, heads * HEAD), lambda _: (part, 0), memory_space=pltpu.VMEM)]
    specs += [vmem] * (2 * blocks)
    if not first:
        specs += [
            pl.BlockSpec(shape, lambda _: (part, 0, 0), memory_space=pltpu.VMEM)
            for shape in (max_shape, sum_shape)
        ]
    pairs = tokens * heads * keys[0].shape[0] * blocks
    return pl.pallas_call(
        functools.partial(attention_kernel, blocks, heads, first, last),
        out_shape=out_shape,
        grid=(1,),
        in_specs=[smem, smem] + specs,
        out_specs=out_specs,
        scratch_shapes=scratch,
        name="attend_last" if last else "attend_first",
        cost_estimate=pl.CostEstimate(
            flops=pairs * 4 * HEAD, bytes_accessed=4 << 20, transcendentals=pairs
        ),
        compiler_params=pltpu.CompilerParams(vmem_limit_bytes=40 << 20),
    )(info, docs, *operands)


def on_device(
    hidden,
    queries,
    norm_gain,
    key_matrix,
    value_matrix,
    key_shift_bias,
    value_shift_bias,
    doc_lengths,
):
    sp_count = lax.axis_size("sp")
    blk_count = lax.axis_size("blk")
    sp_place = lax.axis_index("sp")
    blk_place = lax.axis_index("blk")
    rep_place = lax.axis_index("rep")
    local_rows = hidden.shape[1]
    width = hidden.shape[2]
    span_rows = local_rows * sp_count
    kv_local = key_matrix.shape[1] // HEAD
    quads = sp_count // kv_local
    quad_rows = local_rows * kv_local
    side = blk_place % 2
    half_heads = kv_local // 2
    half_columns = half_heads * HEAD

    near = [[q * kv_local + i for i in range(kv_local)] for q in range(quads)]
    swap = [(b, b ^ 1) for b in range(blk_count)]
    ahead = [(b, (b + 1) % blk_count) for b in range(blk_count)]
    behind = [((b + 1) % blk_count, b) for b in range(blk_count)]

    picked = jnp.concatenate(
        [
            lax.dynamic_slice_in_dim(key_matrix, side * half_columns, half_columns, 1),
            lax.dynamic_slice_in_dim(value_matrix, side * half_columns, half_columns, 1),
        ],
        axis=1,
    )
    weight = lax.all_gather(picked, "sp", axis=0, tiled=True)

    rows_all = hidden[0].astype(jnp.float32)
    row_scale = lax.rsqrt(jnp.mean(rows_all * rows_all, axis=1, keepdims=True) + EPS_VALUE)
    normed = (rows_all * row_scale * norm_gain).astype(jnp.bfloat16)
    half_width = width // 2
    mine = lax.dynamic_slice_in_dim(normed, rep_place * half_width, half_width, 1)
    theirs = lax.ppermute(mine, "blk", swap)
    theirs_other = lax.ppermute(theirs, "rep", [(0, 1), (1, 0)])
    is_low = rep_place == 0
    partner = jnp.concatenate(
        [
            jnp.where(is_low, theirs, theirs_other),
            jnp.where(is_low, theirs_other, theirs),
        ],
        axis=1,
    )
    both = jnp.concatenate([normed, partner], axis=0)

    query_moved = lax.ppermute(queries[0], "blk", behind)
    query = lax.all_to_all(
        query_moved, "sp", split_axis=1, concat_axis=0, tiled=True, axis_index_groups=near
    )

    both, query = lax.optimization_barrier((both, query))
    projected = jnp.dot(both, weight, preferred_element_type=jnp.float32)
    bias = jnp.concatenate(
        [
            lax.dynamic_slice_in_dim(key_shift_bias, side * half_columns, half_columns, 0),
            lax.dynamic_slice_in_dim(value_shift_bias, side * half_columns, half_columns, 0),
        ]
    ).astype(jnp.float32)
    projected = projected + bias
    local_places = sp_place * local_rows + jnp.arange(local_rows)
    places = jnp.concatenate(
        [local_places + blk_place * span_rows, local_places + (blk_place ^ 1) * span_rows]
    )
    keys_new = apply_rotation(
        projected[:, :half_columns].reshape(2 * local_rows, half_heads, HEAD),
        places.astype(jnp.float32),
    ).astype(jnp.bfloat16)
    values_new = (
        projected[:, half_columns:]
        .reshape(2 * local_rows, half_heads, HEAD)
        .astype(jnp.bfloat16)
    )
    pair_new = jnp.concatenate([keys_new, values_new], axis=2).reshape(
        2 * local_rows, half_heads * 2 * HEAD
    )
    kept = pair_new[:local_rows]
    other = lax.ppermute(pair_new[local_rows:], "blk", swap)
    even = side == 0
    all_heads = jnp.concatenate(
        [jnp.where(even, kept, other), jnp.where(even, other, kept)], axis=1
    )
    def to_heads(part):
        one = all_heads.reshape(local_rows, kv_local, 2 * HEAD)[:, :, part * HEAD : (part + 1) * HEAD]
        sent = jnp.tile(one.reshape(local_rows, kv_local * HEAD), (1, quads))
        return lax.all_to_all(sent, "sp", split_axis=1, concat_axis=0, tiled=True)

    key_block = to_heads(0)
    value_block = to_heads(1)
    key_next = lax.ppermute(key_block, "blk", behind)
    key_prior = lax.ppermute(key_block, "blk", ahead)
    value_next = lax.ppermute(value_block, "blk", behind)
    value_prior = lax.ppermute(value_block, "blk", ahead)

    query_block = (blk_place + 1) % blk_count
    base = query_block * span_rows
    query_base = base + sp_place // kv_local * quad_rows
    info_first = jnp.stack([query_base, base - span_rows]).astype(jnp.int32)
    state = attend(info_first, doc_lengths, query, [key_block], [value_block], None, False)
    shares = []
    for part in range(2):
        part_base = query_base + part * (quad_rows // 2)
        info_last = jnp.stack([part_base, base, base - 2 * span_rows]).astype(jnp.int32)
        share = attend(
            info_last,
            doc_lengths,
            query,
            [key_next, key_prior],
            [value_next, value_prior],
            state,
            True,
            part,
            2,
        )
        shares.append(lax.ppermute(share, "blk", ahead))
    spread = lax.all_to_all(
        jnp.concatenate(shares, axis=0),
        "sp",
        split_axis=0,
        concat_axis=1,
        tiled=True,
        axis_index_groups=near,
    )
    return spread[None]


def solution(mesh):
    in_specs = (
        P(("grp", "blk"), "sp", None),
        P(("grp", "blk"), "sp", "rep"),
        P(),
        P("sp", "rep"),
        P("sp", "rep"),
        P("rep"),
        P("rep"),
        P("grp"),
    )
    out_specs = P(("grp", "blk"), "sp", "rep")
    return jax.shard_map(
        on_device, mesh=mesh, in_specs=in_specs, out_specs=out_specs, check_vma=False
    )
```

```python
import functools
import math

import jax
import jax.numpy as jnp
from jax import lax
from jax.experimental import pallas as pl
from jax.experimental.pallas import tpu as pltpu
from jax.sharding import PartitionSpec as P

HEAD = 128
EPS_VALUE = 1e-06
THETA_BASE = 1000000.0
START_MAX = -1e30
HIDDEN_SCORE = -3e38
EXP2_SCALE = math.log2(math.e) / math.sqrt(HEAD)
PIECE = 1024
TILE = 128
LEAD = 2
ROWS = 256


def rotation(token_places):
    half_size = HEAD // 2
    freq_index = jnp.arange(half_size).astype(jnp.float32)
    inverse = jnp.exp(freq_index * (-2.0 * math.log(THETA_BASE) / HEAD))
    angles = token_places[:, None] * inverse[None, :]
    cosine = jnp.cos(angles)
    sine = jnp.sin(angles)
    return jnp.concatenate([cosine, cosine], axis=1), jnp.concatenate([-sine, sine], axis=1)


def project_kernel(heads, tokens_ref, weight_ref, bias_ref, cosine_ref, sine_ref, out_ref, total):
    step = pl.program_id(0)
    product = jnp.dot(tokens_ref[...], weight_ref[...], preferred_element_type=jnp.float32)

    @pl.when(step == 0)
    def _():
        total[...] = product

    @pl.when(step > 0)
    def _():
        total[...] += product

    @pl.when(step == pl.num_programs(0) - 1)
    def _():
        for h in range(heads):
            columns = slice(h * HEAD, (h + 1) * HEAD)
            key = total[:, columns] + bias_ref[:, columns]
            turned = key * cosine_ref[...] + pltpu.roll(key, HEAD // 2, 1) * sine_ref[...]
            out_ref[:, columns] = turned.astype(jnp.bfloat16)
        rest = slice(heads * HEAD, 2 * heads * HEAD)
        out_ref[:, rest] = (total[:, rest] + bias_ref[:, rest]).astype(jnp.bfloat16)


def project(tokens, weight, bias, cosine, sine):
    rows, width = tokens.shape
    columns = weight.shape[1]
    depth = 1024
    whole = lambda shape: pl.BlockSpec(shape, lambda k: (0, 0))
    return pl.pallas_call(
        functools.partial(project_kernel, columns // (2 * HEAD)),
        out_shape=jax.ShapeDtypeStruct((rows, columns), jnp.bfloat16),
        grid=(width // depth,),
        in_specs=[
            pl.BlockSpec((rows, depth), lambda k: (0, k)),
            pl.BlockSpec((depth, columns), lambda k: (k, 0)),
            whole((1, columns)),
            whole((rows, HEAD)),
            whole((rows, HEAD)),
        ],
        out_specs=whole((rows, columns)),
        scratch_shapes=[pltpu.VMEM((rows, columns), jnp.float32)],
        name="project",
        cost_estimate=pl.CostEstimate(
            flops=2 * rows * width * columns,
            bytes_accessed=2 * (rows + columns) * width,
            transcendentals=0,
        ),
        compiler_params=pltpu.CompilerParams(vmem_limit_bytes=58 << 20),
    )(tokens, weight, bias, cosine, sine)


def attention_kernel(blocks, heads, first, last, info, docs, q_ref, *refs):
    keys, values = refs[:blocks], refs[blocks : 2 * blocks]
    rest = list(refs[2 * blocks :])
    if not first:
        max_in, sum_in = rest[0], rest[1]
        rest = rest[2:]
    if last:
        out_ref = rest[0]
        max_ref, sum_ref = rest[1], rest[2]
        rest = rest[3:]
    else:
        max_ref, sum_ref = rest[0], rest[1]
        rest = rest[2:]
    stacked = rest[0]
    bounds = rest[1]
    tiles = q_ref.shape[0] // TILE
    count = docs.shape[0]
    pieces = keys[0].shape[0] // PIECE
    query_base = info[0]

    ends = []
    total = 0
    for d in range(count):
        total = total + docs[d]
        ends.append(total)

    def start_of(place):
        begin = 0
        for end in ends:
            begin = jnp.where(end <= place, end, begin)
        return begin

    for i in range(tiles):
        low = query_base + i * TILE
        bounds[2 * i] = start_of(low)
        bounds[2 * i + 1] = start_of(low + TILE - 1)
        for h in range(heads):
            stacked[i, h * TILE : (h + 1) * TILE, :] = q_ref[
                i * TILE : (i + 1) * TILE, h * HEAD : (h + 1) * HEAD
            ]
    if first:
        max_ref[...] = jnp.full(max_ref.shape, START_MAX, jnp.float32)
        sum_ref[...] = jnp.zeros(sum_ref.shape, jnp.float32)
    else:
        max_ref[...] = max_in[...]
        sum_ref[...] = sum_in[...]

    def step(key_ref, value_ref, piece, i, low, key_low, masked):
        key_rows = pl.ds(pl.multiple_of(piece * PIECE, PIECE), PIECE)
        key = key_ref[key_rows, :]
        value = jnp.concatenate(
            [value_ref[key_rows, :], jnp.ones((PIECE, HEAD), jnp.bfloat16)], axis=1
        )
        visible = None
        if masked:
            row_place = low + lax.broadcasted_iota(jnp.int32, (TILE, HEAD), 0)
            begin = jnp.zeros((TILE, HEAD), jnp.int32)
            for end in ends:
                begin = jnp.where(row_place >= end, end, begin)
            lanes = lax.broadcasted_iota(jnp.int32, (TILE, HEAD), 1)
            parts = []
            for part in range(PIECE // HEAD):
                key_place = lanes + (key_low + part * HEAD)
                parts.append((key_place <= row_place) & (key_place >= begin))
            visible = jnp.concatenate(parts, axis=1)
        chunks = heads * TILE // ROWS

        def scores_of(r):
            scores = lax.dot_general(
                stacked[i, r * ROWS : (r + 1) * ROWS, :],
                key,
                (((1,), (1,)), ((), ())),
                preferred_element_type=jnp.float32,
            )
            if masked:
                scores = jnp.concatenate(
                    [
                        jnp.where(visible, scores[k * TILE : (k + 1) * TILE], HIDDEN_SCORE)
                        for k in range(ROWS // TILE)
                    ],
                    axis=0,
                )
            return scores

        ready = [scores_of(r) for r in range(min(LEAD, chunks))]
        for r in range(chunks):
            rows = slice(r * ROWS, (r + 1) * ROWS)
            scores = ready.pop(0)
            if r + LEAD < chunks:
                ready.append(scores_of(r + LEAD))
            old_max = max_ref[i, rows, :]
            new_max = jnp.maximum(old_max, jnp.max(scores, axis=1, keepdims=True))
            factor = jnp.exp2((old_max - new_max) * EXP2_SCALE)
            weights = jnp.exp2(
                (scores - jnp.concatenate([new_max] * (PIECE // HEAD), axis=1)) * EXP2_SCALE
            ).astype(jnp.bfloat16)
            added = lax.dot_general(
                weights, value, (((1,), (0,)), ((), ())), preferred_element_type=jnp.float32
            )
            sum_ref[i, rows, :] = (
                sum_ref[i, rows, :] * jnp.concatenate([factor, factor], axis=1) + added
            )
            max_ref[i, rows, :] = new_max

    for j in range(blocks):
        key_base = info[1 + j]

        def over_pieces(piece, carry, j=j, key_base=key_base):
            key_low = key_base + piece * PIECE

            def over_tiles(i, inner):
                low = query_base + i * TILE
                reached = (key_low <= low + TILE - 1) & (
                    key_low + PIECE - 1 >= bounds[2 * i]
                )
                whole = (key_low + PIECE - 1 <= low) & (key_low >= bounds[2 * i + 1])

                @pl.when(reached & whole)
                def _():
                    step(keys[j], values[j], piece, i, low, key_low, False)

                @pl.when(reached & jnp.logical_not(whole))
                def _():
                    step(keys[j], values[j], piece, i, low, key_low, True)

                return inner

            return lax.fori_loop(0, tiles, over_tiles, carry)

        lax.fori_loop(0, pieces, over_pieces, 0)

    if last:
        for i in range(tiles):
            for h in range(heads):
                rows = slice(h * TILE, (h + 1) * TILE)
                out_ref[i * TILE : (i + 1) * TILE, h * HEAD : (h + 1) * HEAD] = (
                    sum_ref[i, rows, :HEAD] / sum_ref[i, rows, HEAD:]
                ).astype(jnp.bfloat16)


def attend(info, docs, query, keys, values, state, last, part=0, parts=1):
    tokens = query.shape[0] // parts
    heads = query.shape[1] // HEAD
    tiles = tokens // TILE
    blocks = len(keys)
    first = state is None
    max_shape = (tiles, heads * TILE, HEAD)
    sum_shape = (tiles, heads * TILE, 2 * HEAD)
    vmem = pl.BlockSpec(memory_space=pltpu.VMEM)
    smem = pl.BlockSpec(memory_space=pltpu.SMEM)
    held = [pltpu.VMEM(max_shape, jnp.float32), pltpu.VMEM(sum_shape, jnp.float32)]
    scratch = [
        pltpu.VMEM((tiles, heads * TILE, HEAD), jnp.bfloat16),
        pltpu.SMEM((2 * tiles,), jnp.int32),
    ]
    if last:
        out_shape = jax.ShapeDtypeStruct((tokens, heads * HEAD), jnp.bfloat16)
        out_specs = vmem
        scratch = held + scratch
    else:
        out_shape = (
            jax.ShapeDtypeStruct(max_shape, jnp.float32),
            jax.ShapeDtypeStruct(sum_shape, jnp.float32),
        )
        out_specs = (vmem, vmem)
    operands = [query, *keys, *values] + ([] if first else list(state))
    specs = [pl.BlockSpec((tokens, heads * HEAD), lambda _: (part, 0), memory_space=pltpu.VMEM)]
    specs += [vmem] * (2 * blocks)
    if not first:
        specs += [
            pl.BlockSpec(shape, lambda _: (part, 0, 0), memory_space=pltpu.VMEM)
            for shape in (max_shape, sum_shape)
        ]
    pairs = tokens * heads * keys[0].shape[0] * blocks
    return pl.pallas_call(
        functools.partial(attention_kernel, blocks, heads, first, last),
        out_shape=out_shape,
        grid=(1,),
        in_specs=[smem, smem] + specs,
        out_specs=out_specs,
        scratch_shapes=scratch,
        name="attend_last" if last else "attend_first",
        cost_estimate=pl.CostEstimate(
            flops=pairs * 4 * HEAD, bytes_accessed=4 << 20, transcendentals=pairs
        ),
        compiler_params=pltpu.CompilerParams(vmem_limit_bytes=40 << 20),
    )(info, docs, *operands)


def on_device(
    hidden,
    queries,
    norm_gain,
    key_matrix,
    value_matrix,
    key_shift_bias,
    value_shift_bias,
    doc_lengths,
):
    sp_count = lax.axis_size("sp")
    blk_count = lax.axis_size("blk")
    sp_place = lax.axis_index("sp")
    blk_place = lax.axis_index("blk")
    rep_place = lax.axis_index("rep")
    local_rows = hidden.shape[1]
    width = hidden.shape[2]
    span_rows = local_rows * sp_count
    kv_local = key_matrix.shape[1] // HEAD
    quads = sp_count // kv_local
    quad_rows = local_rows * kv_local
    side = blk_place % 2
    half_heads = kv_local // 2
    half_columns = half_heads * HEAD

    near = [[q * kv_local + i for i in range(kv_local)] for q in range(quads)]
    swap = [(b, b ^ 1) for b in range(blk_count)]
    ahead = [(b, (b + 1) % blk_count) for b in range(blk_count)]
    behind = [((b + 1) % blk_count, b) for b in range(blk_count)]

    picked = jnp.concatenate(
        [
            lax.dynamic_slice_in_dim(key_matrix, side * half_columns, half_columns, 1),
            lax.dynamic_slice_in_dim(value_matrix, side * half_columns, half_columns, 1),
        ],
        axis=1,
    )
    weight = lax.all_gather(picked, "sp", axis=0, tiled=True)

    rows_all = hidden[0].astype(jnp.float32)
    row_scale = lax.rsqrt(jnp.mean(rows_all * rows_all, axis=1, keepdims=True) + EPS_VALUE)
    normed = (rows_all * row_scale * norm_gain).astype(jnp.bfloat16)
    half_width = width // 2
    mine = lax.dynamic_slice_in_dim(normed, rep_place * half_width, half_width, 1)
    theirs = lax.ppermute(mine, "blk", swap)
    theirs_other = lax.ppermute(theirs, "rep", [(0, 1), (1, 0)])
    is_low = rep_place == 0
    partner = jnp.concatenate(
        [
            jnp.where(is_low, theirs, theirs_other),
            jnp.where(is_low, theirs_other, theirs),
        ],
        axis=1,
    )
    both = jnp.concatenate([normed, partner], axis=0)

    query = lax.all_to_all(
        queries[0], "sp", split_axis=1, concat_axis=0, tiled=True, axis_index_groups=near
    )

    bias = jnp.concatenate(
        [
            lax.dynamic_slice_in_dim(key_shift_bias, side * half_columns, half_columns, 0),
            lax.dynamic_slice_in_dim(value_shift_bias, side * half_columns, half_columns, 0),
        ]
    ).astype(jnp.float32)[None]
    local_places = sp_place * local_rows + jnp.arange(local_rows)
    places = jnp.concatenate(
        [local_places + blk_place * span_rows, local_places + (blk_place ^ 1) * span_rows]
    )
    cosine, sine = rotation(places.astype(jnp.float32))
    both, query, bias, cosine, sine = lax.optimization_barrier((both, query, bias, cosine, sine))
    made = project(both, weight, bias, cosine, sine)
    near_half = lax.ppermute(made[:local_rows], "blk", ahead)
    far_half = lax.ppermute(
        made[local_rows:], "blk", [(b, ((b ^ 1) + 1) % blk_count) for b in range(blk_count)]
    )
    odd = side == 1

    def to_heads(part):
        columns = slice(part * half_columns, (part + 1) * half_columns)
        one, two = near_half[:, columns], far_half[:, columns]
        heads = jnp.concatenate([jnp.where(odd, one, two), jnp.where(odd, two, one)], axis=1)
        return lax.all_to_all(
            jnp.tile(heads, (1, quads)), "sp", split_axis=1, concat_axis=0, tiled=True
        )

    key_block = to_heads(0)
    value_block = to_heads(1)
    key_next = lax.ppermute(key_block, "blk", behind)
    key_prior = lax.ppermute(key_block, "blk", ahead)
    value_next = lax.ppermute(value_block, "blk", behind)
    value_prior = lax.ppermute(value_block, "blk", ahead)

    base = blk_place * span_rows
    query_base = base + sp_place // kv_local * quad_rows
    info_first = jnp.stack([query_base, base - span_rows]).astype(jnp.int32)
    info_last = jnp.stack([query_base, base, base - 2 * span_rows]).astype(jnp.int32)
    state = attend(info_first, doc_lengths, query, [key_block], [value_block], None, False)
    result = attend(
        info_last,
        doc_lengths,
        query,
        [key_next, key_prior],
        [value_next, value_prior],
        state,
        True,
    )
    spread = lax.all_to_all(
        result.reshape(kv_local, local_rows, result.shape[1]),
        "sp",
        split_axis=0,
        concat_axis=0,
        tiled=True,
        axis_index_groups=near,
    )
    return jnp.concatenate([spread[i] for i in range(kv_local)], axis=1)[None]


def solution(mesh):
    in_specs = (
        P(("grp", "blk"), "sp", None),
        P(("grp", "blk"), "sp", "rep"),
        P(),
        P("sp", "rep"),
        P("sp", "rep"),
        P("rep"),
        P("rep"),
        P("grp"),
    )
    out_specs = P(("grp", "blk"), "sp", "rep")
    return jax.shard_map(
        on_device, mesh=mesh, in_specs=in_specs, out_specs=out_specs, check_vma=False
    )
```

```python
import functools
import math

import jax
import jax.numpy as jnp
from jax import lax
from jax.experimental import pallas as pl
from jax.experimental.pallas import tpu as pltpu
from jax.sharding import PartitionSpec as P

HEAD = 128
EPS_VALUE = 1e-06
THETA_BASE = 1000000.0
START_MAX = -1e30
HIDDEN_SCORE = -3e38
EXP2_SCALE = math.log2(math.e) / math.sqrt(HEAD)
PIECE = 1024
TILE = 128
LEAD = 2
ROWS = 256


def rotation(token_places):
    half_size = HEAD // 2
    freq_index = jnp.arange(half_size).astype(jnp.float32)
    inverse = jnp.exp(freq_index * (-2.0 * math.log(THETA_BASE) / HEAD))
    angles = token_places[:, None] * inverse[None, :]
    cosine = jnp.cos(angles)
    sine = jnp.sin(angles)
    return jnp.concatenate([cosine, cosine], axis=1), jnp.concatenate([-sine, sine], axis=1)


def project_kernel(
    heads, tokens_ref, weight_ref, bias_ref, cosine_ref, sine_ref, own_ref, other_ref
):
    total = jnp.dot(tokens_ref[...], weight_ref[...], preferred_element_type=jnp.float32)
    half = own_ref.shape[0]
    for h in range(2 * heads):
        columns = slice(h * HEAD, (h + 1) * HEAD)
        made = total[:, columns] + bias_ref[:, columns]
        if h < heads:
            made = made * cosine_ref[...] + pltpu.roll(made, HEAD // 2, 1) * sine_ref[...]
        made = made.astype(jnp.bfloat16)
        own_ref[:, columns] = made[:half]
        other_ref[:, columns] = made[half:]


def project(tokens, weight, bias, cosine, sine):
    rows, width = tokens.shape
    columns = weight.shape[1]
    vmem = pl.BlockSpec(memory_space=pltpu.VMEM)
    return pl.pallas_call(
        functools.partial(project_kernel, columns // (2 * HEAD)),
        out_shape=(jax.ShapeDtypeStruct((rows // 2, columns), jnp.bfloat16),) * 2,
        in_specs=[vmem] * 5,
        out_specs=(vmem, vmem),
        name="project",
        cost_estimate=pl.CostEstimate(
            flops=2 * rows * width * columns,
            bytes_accessed=2 * (rows + columns) * width,
            transcendentals=0,
        ),
        compiler_params=pltpu.CompilerParams(vmem_limit_bytes=24 << 20),
    )(tokens, weight, bias, cosine, sine)


def attention_kernel(blocks, heads, first, last, info, docs, q_ref, *refs):
    keys, values = refs[:blocks], refs[blocks : 2 * blocks]
    rest = list(refs[2 * blocks :])
    if not first:
        max_in, sum_in = rest[0], rest[1]
        rest = rest[2:]
    if last:
        out_ref = rest[0]
        max_ref, sum_ref = rest[1], rest[2]
        rest = rest[3:]
    else:
        max_ref, sum_ref = rest[0], rest[1]
        rest = rest[2:]
    stacked = rest[0]
    bounds = rest[1]
    tiles = q_ref.shape[0] // TILE
    count = docs.shape[0]
    pieces = keys[0].shape[0] // PIECE
    query_base = info[0]

    ends = []
    total = 0
    for d in range(count):
        total = total + docs[d]
        ends.append(total)

    def start_of(place):
        begin = 0
        for end in ends:
            begin = jnp.where(end <= place, end, begin)
        return begin

    for i in range(tiles):
        low = query_base + i * TILE
        bounds[2 * i] = start_of(low)
        bounds[2 * i + 1] = start_of(low + TILE - 1)
        for h in range(heads):
            stacked[i, h * TILE : (h + 1) * TILE, :] = q_ref[
                i * TILE : (i + 1) * TILE, h * HEAD : (h + 1) * HEAD
            ]
    if first:
        max_ref[...] = jnp.full(max_ref.shape, START_MAX, jnp.float32)
        sum_ref[...] = jnp.zeros(sum_ref.shape, jnp.float32)
    else:
        max_ref[...] = max_in[...]
        sum_ref[...] = sum_in[...]

    def step(key_ref, value_ref, piece, i, low, key_low, masked):
        key_rows = pl.ds(pl.multiple_of(piece * PIECE, PIECE), PIECE)
        key = key_ref[key_rows, :]
        value = jnp.concatenate(
            [value_ref[key_rows, :], jnp.ones((PIECE, HEAD), jnp.bfloat16)], axis=1
        )
        visible = None
        if masked:
            row_place = low + lax.broadcasted_iota(jnp.int32, (TILE, HEAD), 0)
            begin = jnp.zeros((TILE, HEAD), jnp.int32)
            for end in ends:
                begin = jnp.where(row_place >= end, end, begin)
            lanes = lax.broadcasted_iota(jnp.int32, (TILE, HEAD), 1)
            parts = []
            for part in range(PIECE // HEAD):
                key_place = lanes + (key_low + part * HEAD)
                parts.append((key_place <= row_place) & (key_place >= begin))
            visible = jnp.concatenate(parts, axis=1)
        chunks = heads * TILE // ROWS

        def scores_of(r):
            scores = lax.dot_general(
                stacked[i, r * ROWS : (r + 1) * ROWS, :],
                key,
                (((1,), (1,)), ((), ())),
                preferred_element_type=jnp.float32,
            )
            if masked:
                scores = jnp.concatenate(
                    [
                        jnp.where(visible, scores[k * TILE : (k + 1) * TILE], HIDDEN_SCORE)
                        for k in range(ROWS // TILE)
                    ],
                    axis=0,
                )
            return scores

        ready = [scores_of(r) for r in range(min(LEAD, chunks))]
        for r in range(chunks):
            rows = slice(r * ROWS, (r + 1) * ROWS)
            scores = ready.pop(0)
            if r + LEAD < chunks:
                ready.append(scores_of(r + LEAD))
            old_max = max_ref[i, rows, :]
            new_max = jnp.maximum(old_max, jnp.max(scores, axis=1, keepdims=True))
            factor = jnp.exp2((old_max - new_max) * EXP2_SCALE)
            weights = jnp.exp2(
                (scores - jnp.concatenate([new_max] * (PIECE // HEAD), axis=1)) * EXP2_SCALE
            ).astype(jnp.bfloat16)
            added = lax.dot_general(
                weights, value, (((1,), (0,)), ((), ())), preferred_element_type=jnp.float32
            )
            sum_ref[i, rows, :] = (
                sum_ref[i, rows, :] * jnp.concatenate([factor, factor], axis=1) + added
            )
            max_ref[i, rows, :] = new_max

    for j in range(blocks):
        key_base = info[1 + j]

        def over_pieces(piece, carry, j=j, key_base=key_base):
            key_low = key_base + piece * PIECE

            def over_tiles(i, inner):
                low = query_base + i * TILE
                reached = (key_low <= low + TILE - 1) & (
                    key_low + PIECE - 1 >= bounds[2 * i]
                )
                whole = (key_low + PIECE - 1 <= low) & (key_low >= bounds[2 * i + 1])

                @pl.when(reached & whole)
                def _():
                    step(keys[j], values[j], piece, i, low, key_low, False)

                @pl.when(reached & jnp.logical_not(whole))
                def _():
                    step(keys[j], values[j], piece, i, low, key_low, True)

                return inner

            return lax.fori_loop(0, tiles, over_tiles, carry)

        lax.fori_loop(0, pieces, over_pieces, 0)

    if last:
        for i in range(tiles):
            for h in range(heads):
                rows = slice(h * TILE, (h + 1) * TILE)
                out_ref[i * TILE : (i + 1) * TILE, h * HEAD : (h + 1) * HEAD] = (
                    sum_ref[i, rows, :HEAD] / sum_ref[i, rows, HEAD:]
                ).astype(jnp.bfloat16)


def attend(info, docs, query, keys, values, state, last):
    tokens = query.shape[0]
    heads = query.shape[1] // HEAD
    tiles = tokens // TILE
    blocks = len(keys)
    first = state is None
    max_shape = (tiles, heads * TILE, HEAD)
    sum_shape = (tiles, heads * TILE, 2 * HEAD)
    vmem = pl.BlockSpec(memory_space=pltpu.VMEM)
    smem = pl.BlockSpec(memory_space=pltpu.SMEM)
    held = [pltpu.VMEM(max_shape, jnp.float32), pltpu.VMEM(sum_shape, jnp.float32)]
    scratch = [
        pltpu.VMEM((tiles, heads * TILE, HEAD), jnp.bfloat16),
        pltpu.SMEM((2 * tiles,), jnp.int32),
    ]
    if last:
        out_shape = jax.ShapeDtypeStruct((tokens, heads * HEAD), jnp.bfloat16)
        out_specs = vmem
        scratch = held + scratch
    else:
        out_shape = (
            jax.ShapeDtypeStruct(max_shape, jnp.float32),
            jax.ShapeDtypeStruct(sum_shape, jnp.float32),
        )
        out_specs = (vmem, vmem)
    operands = [query, *keys, *values] + ([] if first else list(state))
    pairs = tokens * heads * keys[0].shape[0] * blocks
    return pl.pallas_call(
        functools.partial(attention_kernel, blocks, heads, first, last),
        out_shape=out_shape,
        in_specs=[smem, smem] + [vmem] * len(operands),
        out_specs=out_specs,
        scratch_shapes=scratch,
        name="attend_last" if last else "attend_first",
        cost_estimate=pl.CostEstimate(
            flops=pairs * 4 * HEAD, bytes_accessed=4 << 20, transcendentals=pairs
        ),
        compiler_params=pltpu.CompilerParams(vmem_limit_bytes=40 << 20),
    )(info, docs, *operands)


def on_device(
    hidden,
    queries,
    norm_gain,
    key_matrix,
    value_matrix,
    key_shift_bias,
    value_shift_bias,
    doc_lengths,
):
    sp_count = lax.axis_size("sp")
    blk_count = lax.axis_size("blk")
    sp_place = lax.axis_index("sp")
    blk_place = lax.axis_index("blk")
    rep_place = lax.axis_index("rep")
    local_rows = hidden.shape[1]
    width = hidden.shape[2]
    span_rows = local_rows * sp_count
    kv_local = key_matrix.shape[1] // HEAD
    quads = sp_count // kv_local
    quad_rows = local_rows * kv_local
    side = blk_place % 2
    half_heads = kv_local // 2
    half_columns = half_heads * HEAD

    near = [[q * kv_local + i for i in range(kv_local)] for q in range(quads)]
    swap = [(b, b ^ 1) for b in range(blk_count)]
    ahead = [(b, (b + 1) % blk_count) for b in range(blk_count)]
    behind = [((b + 1) % blk_count, b) for b in range(blk_count)]

    picked = jnp.concatenate(
        [
            lax.dynamic_slice_in_dim(key_matrix, side * half_columns, half_columns, 1),
            lax.dynamic_slice_in_dim(value_matrix, side * half_columns, half_columns, 1),
        ],
        axis=1,
    )
    weight = lax.all_gather(picked, "sp", axis=0, tiled=True)

    rows_all = hidden[0].astype(jnp.float32)
    row_scale = lax.rsqrt(jnp.mean(rows_all * rows_all, axis=1, keepdims=True) + EPS_VALUE)
    normed = (rows_all * row_scale * norm_gain).astype(jnp.bfloat16)
    half_width = width // 2
    mine = lax.dynamic_slice_in_dim(normed, rep_place * half_width, half_width, 1)
    theirs = lax.ppermute(mine, "blk", swap)
    theirs_other = lax.ppermute(theirs, "rep", [(0, 1), (1, 0)])
    is_low = rep_place == 0
    partner = jnp.concatenate(
        [
            jnp.where(is_low, theirs, theirs_other),
            jnp.where(is_low, theirs_other, theirs),
        ],
        axis=1,
    )
    both = jnp.concatenate([normed, partner], axis=0)

    query = lax.all_to_all(
        queries[0], "sp", split_axis=1, concat_axis=0, tiled=True, axis_index_groups=near
    )

    bias = jnp.concatenate(
        [
            lax.dynamic_slice_in_dim(key_shift_bias, side * half_columns, half_columns, 0),
            lax.dynamic_slice_in_dim(value_shift_bias, side * half_columns, half_columns, 0),
        ]
    ).astype(jnp.float32)[None]
    local_places = sp_place * local_rows + jnp.arange(local_rows)
    places = jnp.concatenate(
        [local_places + blk_place * span_rows, local_places + (blk_place ^ 1) * span_rows]
    )
    cosine, sine = rotation(places.astype(jnp.float32))
    both, query, bias, cosine, sine = lax.optimization_barrier((both, query, bias, cosine, sine))
    own_made, other_made = project(both, weight, bias, cosine, sine)
    near_half = lax.ppermute(own_made, "blk", ahead)
    far_half = lax.ppermute(
        other_made, "blk", [(b, ((b ^ 1) + 1) % blk_count) for b in range(blk_count)]
    )
    odd = side == 1

    def to_heads(part):
        columns = slice(part * half_columns, (part + 1) * half_columns)
        one, two = near_half[:, columns], far_half[:, columns]
        heads = jnp.concatenate([jnp.where(odd, one, two), jnp.where(odd, two, one)], axis=1)
        return lax.all_to_all(
            jnp.tile(heads, (1, quads)), "sp", split_axis=1, concat_axis=0, tiled=True
        )

    key_block = to_heads(0)
    value_block = to_heads(1)
    key_next = lax.ppermute(key_block, "blk", behind)
    key_prior = lax.ppermute(key_block, "blk", ahead)
    value_next = lax.ppermute(value_block, "blk", behind)
    value_prior = lax.ppermute(value_block, "blk", ahead)

    base = blk_place * span_rows
    query_base = base + sp_place // kv_local * quad_rows
    info_first = jnp.stack([query_base, base - span_rows]).astype(jnp.int32)
    info_last = jnp.stack([query_base, base, base - 2 * span_rows]).astype(jnp.int32)
    state = attend(info_first, doc_lengths, query, [key_block], [value_block], None, False)
    result = attend(
        info_last,
        doc_lengths,
        query,
        [key_next, key_prior],
        [value_next, value_prior],
        state,
        True,
    )
    spread = lax.all_to_all(
        result.reshape(kv_local, local_rows, result.shape[1]),
        "sp",
        split_axis=0,
        concat_axis=0,
        tiled=True,
        axis_index_groups=near,
    )
    return jnp.concatenate([spread[i] for i in range(kv_local)], axis=1)[None]


def solution(mesh):
    in_specs = (
        P(("grp", "blk"), "sp", None),
        P(("grp", "blk"), "sp", "rep"),
        P(),
        P("sp", "rep"),
        P("sp", "rep"),
        P("rep"),
        P("rep"),
        P("grp"),
    )
    out_specs = P(("grp", "blk"), "sp", "rep")
    return jax.shard_map(
        on_device, mesh=mesh, in_specs=in_specs, out_specs=out_specs, check_vma=False
    )
```

```python
import functools
import math

import jax
import jax.numpy as jnp
from jax import lax
from jax.experimental import pallas as pl
from jax.experimental.pallas import tpu as pltpu
from jax.sharding import PartitionSpec as P

HEAD = 128
EPS_VALUE = 1e-06
THETA_BASE = 1000000.0
START_MAX = -1e30
HIDDEN_SCORE = -3e38
EXP2_SCALE = math.log2(math.e) / math.sqrt(HEAD)
PIECE = 512
TILE = 512
LEAD = 1
ROWS = 512


def rotation(token_places):
    half_size = HEAD // 2
    freq_index = jnp.arange(half_size).astype(jnp.float32)
    inverse = jnp.exp(freq_index * (-2.0 * math.log(THETA_BASE) / HEAD))
    angles = token_places[:, None] * inverse[None, :]
    cosine = jnp.cos(angles)
    sine = jnp.sin(angles)
    return jnp.concatenate([cosine, cosine], axis=1), jnp.concatenate([-sine, sine], axis=1)


def project_kernel(
    heads, tokens_ref, weight_ref, bias_ref, cosine_ref, sine_ref, own_ref, other_ref
):
    total = jnp.dot(tokens_ref[...], weight_ref[...], preferred_element_type=jnp.float32)
    half = own_ref.shape[0]
    for h in range(2 * heads):
        columns = slice(h * HEAD, (h + 1) * HEAD)
        made = total[:, columns] + bias_ref[:, columns]
        if h < heads:
            made = made * cosine_ref[...] + pltpu.roll(made, HEAD // 2, 1) * sine_ref[...]
        made = made.astype(jnp.bfloat16)
        own_ref[:, columns] = made[:half]
        other_ref[:, columns] = made[half:]


def project(tokens, weight, bias, cosine, sine):
    rows, width = tokens.shape
    columns = weight.shape[1]
    vmem = pl.BlockSpec(memory_space=pltpu.VMEM)
    return pl.pallas_call(
        functools.partial(project_kernel, columns // (2 * HEAD)),
        out_shape=(jax.ShapeDtypeStruct((rows // 2, columns), jnp.bfloat16),) * 2,
        in_specs=[vmem] * 5,
        out_specs=(vmem, vmem),
        name="project",
        cost_estimate=pl.CostEstimate(
            flops=2 * rows * width * columns,
            bytes_accessed=2 * (rows + columns) * width,
            transcendentals=0,
        ),
        compiler_params=pltpu.CompilerParams(vmem_limit_bytes=24 << 20),
    )(tokens, weight, bias, cosine, sine)


def attention_kernel(blocks, heads, first, last, info, docs, q_ref, *refs):
    keys, values = refs[:blocks], refs[blocks : 2 * blocks]
    rest = list(refs[2 * blocks :])
    if not first:
        max_in, sum_in = rest[0], rest[1]
        rest = rest[2:]
    if last:
        out_ref = rest[0]
        max_ref, sum_ref = rest[1], rest[2]
        rest = rest[3:]
    else:
        max_ref, sum_ref = rest[0], rest[1]
        rest = rest[2:]
    stacked = rest[0]
    bounds = rest[1]
    tiles = q_ref.shape[0] // TILE
    count = docs.shape[0]
    pieces = keys[0].shape[0] // PIECE
    query_base = info[0]

    ends = []
    total = 0
    for d in range(count):
        total = total + docs[d]
        ends.append(total)

    def start_of(place):
        begin = 0
        for end in ends:
            begin = jnp.where(end <= place, end, begin)
        return begin

    for i in range(tiles):
        low = query_base + i * TILE
        bounds[2 * i] = start_of(low)
        bounds[2 * i + 1] = start_of(low + TILE - 1)
        for h in range(heads):
            stacked[i, h * TILE : (h + 1) * TILE, :] = q_ref[
                i * TILE : (i + 1) * TILE, h * HEAD : (h + 1) * HEAD
            ]
    if first:
        max_ref[...] = jnp.full(max_ref.shape, START_MAX, jnp.float32)
        sum_ref[...] = jnp.zeros(sum_ref.shape, jnp.float32)
    else:
        max_ref[...] = max_in[...]
        sum_ref[...] = sum_in[...]

    def step(key_ref, value_ref, piece, i, low, key_low, masked):
        key_rows = pl.ds(pl.multiple_of(piece * PIECE, PIECE), PIECE)
        key = key_ref[key_rows, :]
        value = jnp.concatenate(
            [value_ref[key_rows, :], jnp.ones((PIECE, HEAD), jnp.bfloat16)], axis=1
        )
        visible = None
        if masked:
            row_place = low + lax.broadcasted_iota(jnp.int32, (TILE, HEAD), 0)
            begin = jnp.zeros((TILE, HEAD), jnp.int32)
            for end in ends:
                begin = jnp.where(row_place >= end, end, begin)
            lanes = lax.broadcasted_iota(jnp.int32, (TILE, HEAD), 1)
            parts = []
            for part in range(PIECE // HEAD):
                key_place = lanes + (key_low + part * HEAD)
                parts.append((key_place <= row_place) & (key_place >= begin))
            visible = jnp.concatenate(parts, axis=1)
        chunks = heads * TILE // ROWS

        def scores_of(r):
            scores = lax.dot_general(
                stacked[i, r * ROWS : (r + 1) * ROWS, :],
                key,
                (((1,), (1,)), ((), ())),
                preferred_element_type=jnp.float32,
            )
            if masked:
                scores = jnp.concatenate(
                    [
                        jnp.where(visible, scores[k * TILE : (k + 1) * TILE], HIDDEN_SCORE)
                        for k in range(ROWS // TILE)
                    ],
                    axis=0,
                )
            return scores

        ready = [scores_of(r) for r in range(min(LEAD, chunks))]
        for r in range(chunks):
            rows = slice(r * ROWS, (r + 1) * ROWS)
            scores = ready.pop(0)
            if r + LEAD < chunks:
                ready.append(scores_of(r + LEAD))
            old_max = max_ref[i, rows, :]
            new_max = jnp.maximum(old_max, jnp.max(scores, axis=1, keepdims=True))
            factor = jnp.exp2((old_max - new_max) * EXP2_SCALE)
            weights = jnp.exp2(
                (scores - jnp.concatenate([new_max] * (PIECE // HEAD), axis=1)) * EXP2_SCALE
            ).astype(jnp.bfloat16)
            added = lax.dot_general(
                weights, value, (((1,), (0,)), ((), ())), preferred_element_type=jnp.float32
            )
            sum_ref[i, rows, :] = (
                sum_ref[i, rows, :] * jnp.concatenate([factor, factor], axis=1) + added
            )
            max_ref[i, rows, :] = new_max

    for j in range(blocks):
        key_base = info[1 + j]

        def over_pieces(piece, carry, j=j, key_base=key_base):
            key_low = key_base + piece * PIECE

            def over_tiles(i, inner):
                low = query_base + i * TILE
                reached = (key_low <= low + TILE - 1) & (
                    key_low + PIECE - 1 >= bounds[2 * i]
                )
                whole = (key_low + PIECE - 1 <= low) & (key_low >= bounds[2 * i + 1])

                @pl.when(reached & whole)
                def _():
                    step(keys[j], values[j], piece, i, low, key_low, False)

                @pl.when(reached & jnp.logical_not(whole))
                def _():
                    step(keys[j], values[j], piece, i, low, key_low, True)

                return inner

            return lax.fori_loop(0, tiles, over_tiles, carry)

        lax.fori_loop(0, pieces, over_pieces, 0)

    if last:
        for i in range(tiles):
            for h in range(heads):
                rows = slice(h * TILE, (h + 1) * TILE)
                out_ref[i * TILE : (i + 1) * TILE, h * HEAD : (h + 1) * HEAD] = (
                    sum_ref[i, rows, :HEAD] / sum_ref[i, rows, HEAD:]
                ).astype(jnp.bfloat16)


def attend(info, docs, query, keys, values, state, last):
    tokens = query.shape[0]
    heads = query.shape[1] // HEAD
    tiles = tokens // TILE
    blocks = len(keys)
    first = state is None
    max_shape = (tiles, heads * TILE, HEAD)
    sum_shape = (tiles, heads * TILE, 2 * HEAD)
    vmem = pl.BlockSpec(memory_space=pltpu.VMEM)
    smem = pl.BlockSpec(memory_space=pltpu.SMEM)
    held = [pltpu.VMEM(max_shape, jnp.float32), pltpu.VMEM(sum_shape, jnp.float32)]
    scratch = [
        pltpu.VMEM((tiles, heads * TILE, HEAD), jnp.bfloat16),
        pltpu.SMEM((2 * tiles,), jnp.int32),
    ]
    if last:
        out_shape = jax.ShapeDtypeStruct((tokens, heads * HEAD), jnp.bfloat16)
        out_specs = vmem
        scratch = held + scratch
    else:
        out_shape = (
            jax.ShapeDtypeStruct(max_shape, jnp.float32),
            jax.ShapeDtypeStruct(sum_shape, jnp.float32),
        )
        out_specs = (vmem, vmem)
    operands = [query, *keys, *values] + ([] if first else list(state))
    pairs = tokens * heads * keys[0].shape[0] * blocks
    return pl.pallas_call(
        functools.partial(attention_kernel, blocks, heads, first, last),
        out_shape=out_shape,
        in_specs=[smem, smem] + [vmem] * len(operands),
        out_specs=out_specs,
        scratch_shapes=scratch,
        name="attend_last" if last else "attend_first",
        cost_estimate=pl.CostEstimate(
            flops=pairs * 4 * HEAD, bytes_accessed=4 << 20, transcendentals=pairs
        ),
        compiler_params=pltpu.CompilerParams(vmem_limit_bytes=40 << 20),
    )(info, docs, *operands)


def on_device(
    hidden,
    queries,
    norm_gain,
    key_matrix,
    value_matrix,
    key_shift_bias,
    value_shift_bias,
    doc_lengths,
):
    sp_count = lax.axis_size("sp")
    blk_count = lax.axis_size("blk")
    sp_place = lax.axis_index("sp")
    blk_place = lax.axis_index("blk")
    rep_place = lax.axis_index("rep")
    local_rows = hidden.shape[1]
    width = hidden.shape[2]
    span_rows = local_rows * sp_count
    kv_local = key_matrix.shape[1] // HEAD
    quads = sp_count // kv_local
    quad_rows = local_rows * kv_local
    side = blk_place % 2
    half_heads = kv_local // 2
    half_columns = half_heads * HEAD

    near = [[q * kv_local + i for i in range(kv_local)] for q in range(quads)]
    swap = [(b, b ^ 1) for b in range(blk_count)]
    ahead = [(b, (b + 1) % blk_count) for b in range(blk_count)]
    behind = [((b + 1) % blk_count, b) for b in range(blk_count)]

    picked = jnp.concatenate(
        [
            lax.dynamic_slice_in_dim(key_matrix, side * half_columns, half_columns, 1),
            lax.dynamic_slice_in_dim(value_matrix, side * half_columns, half_columns, 1),
        ],
        axis=1,
    )
    weight = lax.all_gather(picked, "sp", axis=0, tiled=True)

    rows_all = hidden[0].astype(jnp.float32)
    row_scale = lax.rsqrt(jnp.mean(rows_all * rows_all, axis=1, keepdims=True) + EPS_VALUE)
    normed = (rows_all * row_scale * norm_gain).astype(jnp.bfloat16)
    half_width = width // 2
    mine = lax.dynamic_slice_in_dim(normed, rep_place * half_width, half_width, 1)
    theirs = lax.ppermute(mine, "blk", swap)
    theirs_other = lax.ppermute(theirs, "rep", [(0, 1), (1, 0)])
    is_low = rep_place == 0
    partner = jnp.concatenate(
        [
            jnp.where(is_low, theirs, theirs_other),
            jnp.where(is_low, theirs_other, theirs),
        ],
        axis=1,
    )
    both = jnp.concatenate([normed, partner], axis=0)

    query = lax.all_to_all(
        queries[0], "sp", split_axis=1, concat_axis=0, tiled=True, axis_index_groups=near
    )

    bias = jnp.concatenate(
        [
            lax.dynamic_slice_in_dim(key_shift_bias, side * half_columns, half_columns, 0),
            lax.dynamic_slice_in_dim(value_shift_bias, side * half_columns, half_columns, 0),
        ]
    ).astype(jnp.float32)[None]
    local_places = sp_place * local_rows + jnp.arange(local_rows)
    places = jnp.concatenate(
        [local_places + blk_place * span_rows, local_places + (blk_place ^ 1) * span_rows]
    )
    cosine, sine = rotation(places.astype(jnp.float32))
    both, query, bias, cosine, sine = lax.optimization_barrier((both, query, bias, cosine, sine))
    own_made, other_made = project(both, weight, bias, cosine, sine)
    near_half = lax.ppermute(own_made, "blk", ahead)
    far_half = lax.ppermute(
        other_made, "blk", [(b, ((b ^ 1) + 1) % blk_count) for b in range(blk_count)]
    )
    odd = side == 1

    def to_heads(part):
        columns = slice(part * half_columns, (part + 1) * half_columns)
        one, two = near_half[:, columns], far_half[:, columns]
        heads = jnp.concatenate([jnp.where(odd, one, two), jnp.where(odd, two, one)], axis=1)
        return lax.all_to_all(
            jnp.tile(heads, (1, quads)), "sp", split_axis=1, concat_axis=0, tiled=True
        )

    key_block = to_heads(0)
    value_block = to_heads(1)
    key_next = lax.ppermute(key_block, "blk", behind)
    key_prior = lax.ppermute(key_block, "blk", ahead)
    value_next = lax.ppermute(value_block, "blk", behind)
    value_prior = lax.ppermute(value_block, "blk", ahead)

    base = blk_place * span_rows
    query_base = base + sp_place // kv_local * quad_rows
    info_first = jnp.stack([query_base, base - span_rows]).astype(jnp.int32)
    info_last = jnp.stack([query_base, base, base - 2 * span_rows]).astype(jnp.int32)
    state = attend(info_first, doc_lengths, query, [key_block], [value_block], None, False)
    result = attend(
        info_last,
        doc_lengths,
        query,
        [key_next, key_prior],
        [value_next, value_prior],
        state,
        True,
    )
    spread = lax.all_to_all(
        result.reshape(kv_local, local_rows, result.shape[1]),
        "sp",
        split_axis=0,
        concat_axis=0,
        tiled=True,
        axis_index_groups=near,
    )
    return jnp.concatenate([spread[i] for i in range(kv_local)], axis=1)[None]


def solution(mesh):
    in_specs = (
        P(("grp", "blk"), "sp", None),
        P(("grp", "blk"), "sp", "rep"),
        P(),
        P("sp", "rep"),
        P("sp", "rep"),
        P("rep"),
        P("rep"),
        P("grp"),
    )
    out_specs = P(("grp", "blk"), "sp", "rep")
    return jax.shard_map(
        on_device, mesh=mesh, in_specs=in_specs, out_specs=out_specs, check_vma=False
    )
```

```python
import functools
import math

import jax
import jax.numpy as jnp
from jax import lax
from jax.experimental import pallas as pl
from jax.experimental.pallas import tpu as pltpu
from jax.sharding import PartitionSpec as P

HEAD = 128
EPS_VALUE = 1e-06
THETA_BASE = 1000000.0
START_MAX = -1e30
HIDDEN_SCORE = -3e38
EXP2_SCALE = math.log2(math.e) / math.sqrt(HEAD)
PIECE = 1024
CUT = 512
TILE = 512
LEAD = 2
ROWS = 512


def rotation(token_places):
    half_size = HEAD // 2
    freq_index = jnp.arange(half_size).astype(jnp.float32)
    inverse = jnp.exp(freq_index * (-2.0 * math.log(THETA_BASE) / HEAD))
    angles = token_places[:, None] * inverse[None, :]
    cosine = jnp.cos(angles)
    sine = jnp.sin(angles)
    return jnp.concatenate([cosine, cosine], axis=1), jnp.concatenate([-sine, sine], axis=1)


def project_kernel(
    heads, tokens_ref, weight_ref, bias_ref, cosine_ref, sine_ref, own_ref, other_ref
):
    total = jnp.dot(tokens_ref[...], weight_ref[...], preferred_element_type=jnp.float32)
    half = own_ref.shape[0]
    for h in range(2 * heads):
        columns = slice(h * HEAD, (h + 1) * HEAD)
        made = total[:, columns] + bias_ref[:, columns]
        if h < heads:
            made = made * cosine_ref[...] + pltpu.roll(made, HEAD // 2, 1) * sine_ref[...]
        made = made.astype(jnp.bfloat16)
        own_ref[:, columns] = made[:half]
        other_ref[:, columns] = made[half:]


def project(tokens, weight, bias, cosine, sine):
    rows, width = tokens.shape
    columns = weight.shape[1]
    vmem = pl.BlockSpec(memory_space=pltpu.VMEM)
    return pl.pallas_call(
        functools.partial(project_kernel, columns // (2 * HEAD)),
        out_shape=(jax.ShapeDtypeStruct((rows // 2, columns), jnp.bfloat16),) * 2,
        in_specs=[vmem] * 5,
        out_specs=(vmem, vmem),
        name="project",
        cost_estimate=pl.CostEstimate(
            flops=2 * rows * width * columns,
            bytes_accessed=2 * (rows + columns) * width,
            transcendentals=0,
        ),
        compiler_params=pltpu.CompilerParams(vmem_limit_bytes=24 << 20),
    )(tokens, weight, bias, cosine, sine)


def attention_kernel(blocks, heads, first, last, info, docs, q_ref, *refs):
    keys, values = refs[:blocks], refs[blocks : 2 * blocks]
    rest = list(refs[2 * blocks :])
    if not first:
        max_in, sum_in = rest[0], rest[1]
        rest = rest[2:]
    if last:
        out_ref = rest[0]
        max_ref, sum_ref = rest[1], rest[2]
        rest = rest[3:]
    else:
        max_ref, sum_ref = rest[0], rest[1]
        rest = rest[2:]
    stacked = rest[0]
    bounds = rest[1]
    tiles = q_ref.shape[0] // TILE
    count = docs.shape[0]
    pieces = keys[0].shape[0] // PIECE
    query_base = info[0]

    ends = []
    total = 0
    for d in range(count):
        total = total + docs[d]
        ends.append(total)

    def start_of(place):
        begin = 0
        for end in ends:
            begin = jnp.where(end <= place, end, begin)
        return begin

    for i in range(tiles):
        low = query_base + i * TILE
        bounds[2 * i] = start_of(low)
        bounds[2 * i + 1] = start_of(low + TILE - 1)
        for h in range(heads):
            stacked[i, h * TILE : (h + 1) * TILE, :] = q_ref[
                i * TILE : (i + 1) * TILE, h * HEAD : (h + 1) * HEAD
            ]
    if first:
        max_ref[...] = jnp.full(max_ref.shape, START_MAX, jnp.float32)
        sum_ref[...] = jnp.zeros(sum_ref.shape, jnp.float32)
    else:
        max_ref[...] = max_in[...]
        sum_ref[...] = sum_in[...]

    def step(key_ref, value_ref, at, size, i, low, key_low, masked):
        key_rows = pl.ds(pl.multiple_of(at, size), size)
        key = key_ref[key_rows, :]
        value = jnp.concatenate(
            [value_ref[key_rows, :], jnp.ones((size, HEAD), jnp.bfloat16)], axis=1
        )
        visible = None
        if masked:
            row_place = low + lax.broadcasted_iota(jnp.int32, (TILE, HEAD), 0)
            begin = jnp.zeros((TILE, HEAD), jnp.int32)
            for end in ends:
                begin = jnp.where(row_place >= end, end, begin)
            lanes = lax.broadcasted_iota(jnp.int32, (TILE, HEAD), 1)
            parts = []
            for part in range(size // HEAD):
                key_place = lanes + (key_low + part * HEAD)
                parts.append((key_place <= row_place) & (key_place >= begin))
            visible = jnp.concatenate(parts, axis=1)
        chunks = heads * TILE // ROWS

        def scores_of(r):
            scores = lax.dot_general(
                stacked[i, r * ROWS : (r + 1) * ROWS, :],
                key,
                (((1,), (1,)), ((), ())),
                preferred_element_type=jnp.float32,
            )
            if masked:
                scores = jnp.concatenate(
                    [
                        jnp.where(visible, scores[k * TILE : (k + 1) * TILE], HIDDEN_SCORE)
                        for k in range(ROWS // TILE)
                    ],
                    axis=0,
                )
            return scores

        ready = [scores_of(r) for r in range(min(LEAD, chunks))]
        for r in range(chunks):
            rows = slice(r * ROWS, (r + 1) * ROWS)
            scores = ready.pop(0)
            if r + LEAD < chunks:
                ready.append(scores_of(r + LEAD))
            old_max = max_ref[i, rows, :]
            new_max = jnp.maximum(old_max, jnp.max(scores, axis=1, keepdims=True))
            factor = jnp.exp2((old_max - new_max) * EXP2_SCALE)
            weights = jnp.exp2(
                (scores - jnp.concatenate([new_max] * (size // HEAD), axis=1)) * EXP2_SCALE
            ).astype(jnp.bfloat16)
            added = lax.dot_general(
                weights, value, (((1,), (0,)), ((), ())), preferred_element_type=jnp.float32
            )
            sum_ref[i, rows, :] = (
                sum_ref[i, rows, :] * jnp.concatenate([factor, factor], axis=1) + added
            )
            max_ref[i, rows, :] = new_max

    for j in range(blocks):
        key_base = info[1 + j]

        def over_pieces(piece, carry, j=j, key_base=key_base):
            key_low = key_base + piece * PIECE

            def over_tiles(i, inner):
                low = query_base + i * TILE
                start_low, start_high = bounds[2 * i], bounds[2 * i + 1]

                def kinds(first_key, size):
                    last_key = first_key + size - 1
                    reached = (first_key <= low + TILE - 1) & (last_key >= start_low)
                    return reached, (last_key <= low) & (first_key >= start_high)

                _, all_whole = kinds(key_low, PIECE)

                @pl.when(all_whole)
                def _():
                    step(keys[j], values[j], piece * PIECE, PIECE, i, low, key_low, False)

                def over_cuts(half, inmost):
                    half_low = key_low + half * CUT
                    at = piece * PIECE + half * CUT
                    reached, whole = kinds(half_low, CUT)
                    reached = reached & jnp.logical_not(all_whole)

                    @pl.when(reached & whole)
                    def _():
                        step(keys[j], values[j], at, CUT, i, low, half_low, False)

                    @pl.when(reached & jnp.logical_not(whole))
                    def _():
                        step(keys[j], values[j], at, CUT, i, low, half_low, True)

                    return inmost

                lax.fori_loop(0, PIECE // CUT, over_cuts, 0)
                return inner

            return lax.fori_loop(0, tiles, over_tiles, carry)

        lax.fori_loop(0, pieces, over_pieces, 0)

    if last:
        for i in range(tiles):
            for h in range(heads):
                rows = slice(h * TILE, (h + 1) * TILE)
                out_ref[i * TILE : (i + 1) * TILE, h * HEAD : (h + 1) * HEAD] = (
                    sum_ref[i, rows, :HEAD] / sum_ref[i, rows, HEAD:]
                ).astype(jnp.bfloat16)


def attend(info, docs, query, keys, values, state, last):
    tokens = query.shape[0]
    heads = query.shape[1] // HEAD
    tiles = tokens // TILE
    blocks = len(keys)
    first = state is None
    max_shape = (tiles, heads * TILE, HEAD)
    sum_shape = (tiles, heads * TILE, 2 * HEAD)
    vmem = pl.BlockSpec(memory_space=pltpu.VMEM)
    smem = pl.BlockSpec(memory_space=pltpu.SMEM)
    held = [pltpu.VMEM(max_shape, jnp.float32), pltpu.VMEM(sum_shape, jnp.float32)]
    scratch = [
        pltpu.VMEM((tiles, heads * TILE, HEAD), jnp.bfloat16),
        pltpu.SMEM((2 * tiles,), jnp.int32),
    ]
    if last:
        out_shape = jax.ShapeDtypeStruct((tokens, heads * HEAD), jnp.bfloat16)
        out_specs = vmem
        scratch = held + scratch
    else:
        out_shape = (
            jax.ShapeDtypeStruct(max_shape, jnp.float32),
            jax.ShapeDtypeStruct(sum_shape, jnp.float32),
        )
        out_specs = (vmem, vmem)
    operands = [query, *keys, *values] + ([] if first else list(state))
    pairs = tokens * heads * keys[0].shape[0] * blocks
    return pl.pallas_call(
        functools.partial(attention_kernel, blocks, heads, first, last),
        out_shape=out_shape,
        in_specs=[smem, smem] + [vmem] * len(operands),
        out_specs=out_specs,
        scratch_shapes=scratch,
        name="attend_last" if last else "attend_first",
        cost_estimate=pl.CostEstimate(
            flops=pairs * 4 * HEAD, bytes_accessed=4 << 20, transcendentals=pairs
        ),
        compiler_params=pltpu.CompilerParams(vmem_limit_bytes=40 << 20),
    )(info, docs, *operands)


def on_device(
    hidden,
    queries,
    norm_gain,
    key_matrix,
    value_matrix,
    key_shift_bias,
    value_shift_bias,
    doc_lengths,
):
    sp_count = lax.axis_size("sp")
    blk_count = lax.axis_size("blk")
    sp_place = lax.axis_index("sp")
    blk_place = lax.axis_index("blk")
    rep_place = lax.axis_index("rep")
    local_rows = hidden.shape[1]
    width = hidden.shape[2]
    span_rows = local_rows * sp_count
    kv_local = key_matrix.shape[1] // HEAD
    quads = sp_count // kv_local
    quad_rows = local_rows * kv_local
    side = blk_place % 2
    half_heads = kv_local // 2
    half_columns = half_heads * HEAD

    near = [[q * kv_local + i for i in range(kv_local)] for q in range(quads)]
    swap = [(b, b ^ 1) for b in range(blk_count)]
    ahead = [(b, (b + 1) % blk_count) for b in range(blk_count)]
    behind = [((b + 1) % blk_count, b) for b in range(blk_count)]

    picked = jnp.concatenate(
        [
            lax.dynamic_slice_in_dim(key_matrix, side * half_columns, half_columns, 1),
            lax.dynamic_slice_in_dim(value_matrix, side * half_columns, half_columns, 1),
        ],
        axis=1,
    )
    weight = lax.all_gather(picked, "sp", axis=0, tiled=True)

    rows_all = hidden[0].astype(jnp.float32)
    row_scale = lax.rsqrt(jnp.mean(rows_all * rows_all, axis=1, keepdims=True) + EPS_VALUE)
    normed = (rows_all * row_scale * norm_gain).astype(jnp.bfloat16)
    half_width = width // 2
    mine = lax.dynamic_slice_in_dim(normed, rep_place * half_width, half_width, 1)
    theirs = lax.ppermute(mine, "blk", swap)
    theirs_other = lax.ppermute(theirs, "rep", [(0, 1), (1, 0)])
    is_low = rep_place == 0
    partner = jnp.concatenate(
        [
            jnp.where(is_low, theirs, theirs_other),
            jnp.where(is_low, theirs_other, theirs),
        ],
        axis=1,
    )
    both = jnp.concatenate([normed, partner], axis=0)

    query = lax.all_to_all(
        queries[0], "sp", split_axis=1, concat_axis=0, tiled=True, axis_index_groups=near
    )

    bias = jnp.concatenate(
        [
            lax.dynamic_slice_in_dim(key_shift_bias, side * half_columns, half_columns, 0),
            lax.dynamic_slice_in_dim(value_shift_bias, side * half_columns, half_columns, 0),
        ]
    ).astype(jnp.float32)[None]
    local_places = sp_place * local_rows + jnp.arange(local_rows)
    places = jnp.concatenate(
        [local_places + blk_place * span_rows, local_places + (blk_place ^ 1) * span_rows]
    )
    cosine, sine = rotation(places.astype(jnp.float32))
    both, query, bias, cosine, sine = lax.optimization_barrier((both, query, bias, cosine, sine))
    own_made, other_made = project(both, weight, bias, cosine, sine)
    near_half = lax.ppermute(own_made, "blk", ahead)
    far_half = lax.ppermute(
        other_made, "blk", [(b, ((b ^ 1) + 1) % blk_count) for b in range(blk_count)]
    )
    odd = side == 1

    def to_heads(part):
        columns = slice(part * half_columns, (part + 1) * half_columns)
        one, two = near_half[:, columns], far_half[:, columns]
        heads = jnp.concatenate([jnp.where(odd, one, two), jnp.where(odd, two, one)], axis=1)
        return lax.all_to_all(
            jnp.tile(heads, (1, quads)), "sp", split_axis=1, concat_axis=0, tiled=True
        )

    key_block = to_heads(0)
    value_block = to_heads(1)
    key_next = lax.ppermute(key_block, "blk", behind)
    key_prior = lax.ppermute(key_block, "blk", ahead)
    value_next = lax.ppermute(value_block, "blk", behind)
    value_prior = lax.ppermute(value_block, "blk", ahead)

    base = blk_place * span_rows
    query_base = base + sp_place // kv_local * quad_rows
    info_first = jnp.stack([query_base, base - span_rows]).astype(jnp.int32)
    info_last = jnp.stack([query_base, base, base - 2 * span_rows]).astype(jnp.int32)
    state = attend(info_first, doc_lengths, query, [key_block], [value_block], None, False)
    result = attend(
        info_last,
        doc_lengths,
        query,
        [key_next, key_prior],
        [value_next, value_prior],
        state,
        True,
    )
    spread = lax.all_to_all(
        result.reshape(kv_local, local_rows, result.shape[1]),
        "sp",
        split_axis=0,
        concat_axis=0,
        tiled=True,
        axis_index_groups=near,
    )
    return jnp.concatenate([spread[i] for i in range(kv_local)], axis=1)[None]


def solution(mesh):
    in_specs = (
        P(("grp", "blk"), "sp", None),
        P(("grp", "blk"), "sp", "rep"),
        P(),
        P("sp", "rep"),
        P("sp", "rep"),
        P("rep"),
        P("rep"),
        P("grp"),
    )
    out_specs = P(("grp", "blk"), "sp", "rep")
    return jax.shard_map(
        on_device, mesh=mesh, in_specs=in_specs, out_specs=out_specs, check_vma=False
    )
```
